8 devices in a mesh: rep: 1 (over z), tp: 2 (over y), ep: 4 (over x, core).
Axes of the slice: x: 2, y: 2, z: 1, core: 2. Of those that a mesh axis runs over, the one named last changes fastest.
Arguments:
- hidden: bfloat16 [512, 2048], P(('rep', 'ep'))
- g_attn: float32 [2048], replicated
- w_q: bfloat16 [2048, 2048], P(None, 'tp')
- w_k: bfloat16 [2048, 512], P(None, 'tp')
- w_v: bfloat16 [2048, 512], P(None, 'tp')
- w_o: bfloat16 [2048, 2048], P('tp')
- k_cache: bfloat16 [512, 256, 4, 128], P(('rep', 'ep'), None, 'tp')
- v_cache: bfloat16 [512, 256, 4, 128], P(('rep', 'ep'), None, 'tp')
- lengths: int32 [512], P(('rep', 'ep'))
- g_ffn: float32 [2048], replicated
- ws_gate: bfloat16 [2048, 2816], P(None, 'tp')
- ws_up: bfloat16 [2048, 2816], P(None, 'tp')
- ws_down: bfloat16 [2816, 2048], P('tp')
- w_gate: bfloat16 [64, 2048, 1408], P(('ep', 'tp'))
- w_up: bfloat16 [64, 2048, 1408], P(('ep', 'tp'))
- w_down: bfloat16 [64, 1408, 2048], P(('ep', 'tp'))
- expert_ids: int32 [512, 6], P(('rep', 'ep'))
- gate_vals: float32 [512, 6], P(('rep', 'ep'))
Outputs:
- output: bfloat16 [512, 2048], P(('rep', 'ep'))
All inputs are finite; a program needn't handle non-finite values.
Results may differ from the reference program's by a relative error of at most 0.0135975.
Values are sent between devices in bfloat16 or wider.
A program may use at most 1 GiB of HBM per device.

```python
import jax
import jax.numpy as jnp
from jax import lax

D = 2048
HQ = 16
HKV = 4
HEAD = 128
EXPERTS = 64
TOP = 6
FF = 1408
FS = 2816
EP = 4
TOK = 128
CTX = 256

NTOK = EP * TOK
GROUP = HQ // HKV
SLOT = min(TOK, (2 * TOK * TOP + EXPERTS - 1) // EXPERTS)
EPS = 1e-6


def rms_norm(values, gain):
    return values * lax.rsqrt(jnp.mean(values * values, axis=-1, keepdims=True) + EPS) * gain


def normal_bf16(rng_key, arr_shape, factor):
    return (jax.random.normal(rng_key, arr_shape, jnp.float32) * factor).astype(jnp.bfloat16)


def draw_routes(rng_key):
    key_keep, key_label, key_order = jax.random.split(rng_key, 3)
    slot_total = EXPERTS * SLOT
    shuffled = jax.random.permutation(key_keep, slot_total - SLOT)
    kept_mask = jnp.concatenate([jnp.ones((SLOT,), dtype=bool), shuffled < TOK * TOP - SLOT])
    position = jnp.arange(slot_total)
    kept_order = jnp.argsort(jnp.where(kept_mask, position, position + slot_total))
    labels = kept_order[: TOK * TOP] // SLOT
    choice_table = labels.reshape(TOP, TOK).T
    relabel = jax.random.permutation(key_label, EXPERTS)
    token_order = jax.random.permutation(key_order, TOK)
    return relabel[choice_table][token_order].astype(jnp.int32)


def draw_lengths(rng_key):
    key_base, key_first, key_second = jax.random.split(rng_key, 3)
    low_len = CTX // 8
    base_len = jax.random.randint(key_base, (NTOK,), low_len, CTX + 1)
    first_pos = jax.random.randint(key_first, (), 0, NTOK)
    second_pos = (first_pos + 1 + jax.random.randint(key_second, (), 0, NTOK - 1)) % NTOK
    token_pos = jnp.arange(NTOK)
    base_len = jnp.where(token_pos == first_pos, CTX, base_len)
    base_len = jnp.where(token_pos == second_pos, low_len, base_len)
    return base_len.astype(jnp.int32)


def setup_inputs(seed: int = 0, part: int = 0) -> dict:
    key_list = jax.random.split(jax.random.key(seed), 18)
    k_hidden = jax.random.fold_in(key_list[0], part)
    k_kcache = jax.random.fold_in(key_list[6], part)
    k_vcache = jax.random.fold_in(key_list[7], part)
    k_lengths = jax.random.fold_in(key_list[8], part)
    k_routes = jax.random.fold_in(key_list[16], part)
    k_gates = jax.random.fold_in(key_list[17], part)
    return {
        'hidden': normal_bf16(k_hidden, (NTOK, D), 1.0),
        'g_attn': 1.0 + 0.2 * jax.random.normal(key_list[1], (D,), jnp.float32),
        'w_q': normal_bf16(key_list[2], (D, HQ * HEAD), D ** -0.5),
        'w_k': normal_bf16(key_list[3], (D, HKV * HEAD), D ** -0.5),
        'w_v': normal_bf16(key_list[4], (D, HKV * HEAD), (CTX / (2.0 * D)) ** 0.5),
        'w_o': normal_bf16(key_list[5], (HQ * HEAD, D), (CTX / (8.0 * HQ * HEAD)) ** 0.5),
        'k_cache': normal_bf16(k_kcache, (NTOK, CTX, HKV, HEAD), 1.0),
        'v_cache': normal_bf16(k_vcache, (NTOK, CTX, HKV, HEAD), 1.0),
        'lengths': draw_lengths(k_lengths),
        'g_ffn': 1.0 + 0.2 * jax.random.normal(key_list[9], (D,), jnp.float32),
        'ws_gate': normal_bf16(key_list[10], (D, FS), D ** -0.5),
        'ws_up': normal_bf16(key_list[11], (D, FS), D ** -0.5),
        'ws_down': normal_bf16(key_list[12], (FS, D), 1.5 * FS ** -0.5),
        'w_gate': normal_bf16(key_list[13], (EXPERTS, D, FF), D ** -0.5),
        'w_up': normal_bf16(key_list[14], (EXPERTS, D, FF), D ** -0.5),
        'w_down': normal_bf16(key_list[15], (EXPERTS, FF, D), 1.5 * FF ** -0.5),
        'expert_ids': jax.vmap(draw_routes)(jax.random.split(k_routes, EP)).reshape(NTOK, TOP),
        'gate_vals': jnp.exp(0.5 * jax.random.normal(k_gates, (NTOK, TOP), jnp.float32)) * TOP ** -0.5,
    }


def reference(hidden, g_attn, w_q, w_k, w_v, w_o, k_cache, v_cache, lengths, g_ffn, ws_gate, ws_up, ws_down, w_gate, w_up, w_down, expert_ids, gate_vals):
    h_f32 = hidden.astype(jnp.float32)
    x_norm = rms_norm(h_f32, g_attn).astype(jnp.bfloat16)
    queries = jnp.dot(x_norm, w_q, preferred_element_type=jnp.float32).astype(jnp.bfloat16)
    k_new = jnp.dot(x_norm, w_k, preferred_element_type=jnp.float32).astype(jnp.bfloat16)
    v_new = jnp.dot(x_norm, w_v, preferred_element_type=jnp.float32).astype(jnp.bfloat16)
    score_scale = HEAD ** -0.5

    def attend(token_args):
        q_row, kn_row, vn_row, k_rows, v_rows, length = token_args
        q_grp = q_row.reshape(HKV, GROUP, HEAD).astype(jnp.float32)
        kn_f32 = kn_row.reshape(HKV, HEAD).astype(jnp.float32)
        vn_f32 = vn_row.reshape(HKV, HEAD).astype(jnp.float32)
        scores = jnp.einsum('kgd,skd->kgs', q_grp, k_rows.astype(jnp.float32)) * score_scale
        scores = jnp.where(jnp.arange(CTX) < length, scores, -jnp.inf)
        self_score = jnp.einsum('kgd,kd->kg', q_grp, kn_f32) * score_scale
        top_score = jnp.maximum(jnp.max(scores, axis=-1), self_score)
        weights = jnp.exp(scores - top_score[:, :, None])
        self_weight = jnp.exp(self_score - top_score)
        norm_sum = jnp.sum(weights, axis=-1) + self_weight
        mixed_sum = jnp.einsum('kgs,skd->kgd', weights.astype(jnp.bfloat16).astype(jnp.float32), v_rows.astype(jnp.float32))
        self_term = self_weight.astype(jnp.bfloat16).astype(jnp.float32)[:, :, None] * vn_f32[:, None, :]
        return ((mixed_sum + self_term) / norm_sum[:, :, None]).astype(jnp.bfloat16).reshape(HQ * HEAD)

    heads_out = lax.map(attend, (queries, k_new, v_new, k_cache, v_cache, lengths))
    attn = jnp.dot(heads_out, w_o, preferred_element_type=jnp.float32).astype(jnp.bfloat16)
    attn_f32 = attn.astype(jnp.float32)
    y_norm = rms_norm(h_f32 + attn_f32, g_ffn).astype(jnp.bfloat16)
    shared_act = jax.nn.silu(jnp.dot(y_norm, ws_gate, preferred_element_type=jnp.float32)) * jnp.dot(y_norm, ws_up, preferred_element_type=jnp.float32)
    shared = jnp.dot(shared_act.astype(jnp.bfloat16), ws_down, preferred_element_type=jnp.float32)
    onehot = expert_ids[:, :, None] == jnp.arange(EXPERTS)
    picked = jnp.any(onehot, axis=1)
    gate_mat = jnp.sum(jnp.where(onehot, gate_vals[:, :, None], 0.0), axis=1)
    row_cap = EP * SLOT

    def expert_step(routed_acc, expert_args):
        w_g, w_u, w_d, col_pick, col_gate = expert_args
        row_idx = jnp.nonzero(col_pick, size=row_cap, fill_value=0)[0]
        row_valid = jnp.arange(row_cap) < jnp.sum(col_pick)
        row_gate = jnp.where(row_valid, col_gate[row_idx], 0.0)
        x_rows = x_norm[row_idx]
        expert_act = jax.nn.silu(jnp.dot(x_rows, w_g, preferred_element_type=jnp.float32)) * jnp.dot(x_rows, w_u, preferred_element_type=jnp.float32)
        y_rows = jnp.dot(expert_act.astype(jnp.bfloat16), w_d, preferred_element_type=jnp.float32) * row_gate[:, None]
        return routed_acc.at[row_idx].add(y_rows), None

    routed = lax.scan(expert_step, jnp.zeros((NTOK, D), jnp.float32), (w_gate, w_up, w_down, picked.T, gate_mat.T))[0]
    return (h_f32 + attn_f32 + shared + routed).astype(jnp.bfloat16)
```

```python
import functools

import jax
import jax.numpy as jnp
from jax import lax
from jax.experimental import pallas as pl
from jax.experimental.pallas import tpu as pltpu
from jax.sharding import PartitionSpec as P

EPS = 1e-6
TILE = 256
SLOT = 32
MESH_ID = pl.DeviceIdType.MESH


def rms_norm(values, gain):
    return values * lax.rsqrt(jnp.mean(values * values, axis=-1, keepdims=True) + EPS) * gain


def attention_heads(x_norm, w_q, w_k, w_v, k_cache, v_cache, lengths):
    tokens, ctx_len, kv_heads, head_dim = k_cache.shape
    q_heads = w_q.shape[1] // head_dim
    group_size = q_heads // kv_heads
    score_scale = head_dim ** -0.5
    queries = jnp.dot(x_norm, w_q, preferred_element_type=jnp.float32).astype(jnp.bfloat16).reshape(tokens, kv_heads, group_size, head_dim)
    k_new = jnp.dot(x_norm, w_k, preferred_element_type=jnp.float32).astype(jnp.bfloat16).reshape(tokens, kv_heads, head_dim)
    v_new = jnp.dot(x_norm, w_v, preferred_element_type=jnp.float32).astype(jnp.bfloat16).reshape(tokens, kv_heads, head_dim)
    scores = jnp.einsum('tkgd,tskd->tkgs', queries, k_cache, preferred_element_type=jnp.float32) * score_scale
    valid_pos = jnp.arange(ctx_len)[None, None, None, :] < lengths[:, None, None, None]
    scores = jnp.where(valid_pos, scores, -jnp.inf)
    self_score = jnp.einsum('tkgd,tkd->tkg', queries, k_new, preferred_element_type=jnp.float32) * score_scale
    top_score = jnp.maximum(jnp.max(scores, axis=-1), self_score)
    weights = jnp.exp(scores - top_score[..., None])
    self_weight = jnp.exp(self_score - top_score)
    norm_sum = jnp.sum(weights, axis=-1) + self_weight
    mixed_sum = jnp.einsum('tkgs,tskd->tkgd', weights.astype(jnp.bfloat16), v_cache, preferred_element_type=jnp.float32)
    self_term = self_weight.astype(jnp.bfloat16).astype(jnp.float32)[..., None] * v_new.astype(jnp.float32)[:, :, None, :]
    heads_out = ((mixed_sum + self_term) / norm_sum[..., None]).astype(jnp.bfloat16)
    return heads_out.reshape(tokens, q_heads * head_dim)


def gate_table(expert_ids, gate_vals, num_experts):
    onehot = expert_ids[:, :, None] == jnp.arange(num_experts)
    return jnp.sum(jnp.where(onehot, gate_vals[:, :, None], 0.0), axis=1).T


def moe_kernel(x_ref, attn_ref, h_ref, gt_ref, gain_ref, wsg_ref, wsu_ref, wsd_ref, wg_ref, wu_ref, wd_ref, out_ref,
               x_all, x_rows, act, place_t, slot_gate, place, y_rows, ring, down, attn_rx, attn_sum, y_norm, gates,
               send1, recv1, send2, recv2, send3, recv3, keep_own, keep_other,
               ring_sem, down_sem, x_ssem, x_rsem, g_ssem, g_rsem, a_sem, s1_sem, r1_sem, s2_sem, r2_sem, s3_sem, r3_sem):
    tp = lax.axis_index('tp')
    ep = lax.axis_index('ep')
    core = ep % 2
    chip = ep // 2
    mate = chip * 2 + 1 - core
    across = (1 - chip) * 2 + core
    diagonal = (1 - chip) * 2 + 1 - core
    tokens, d_model = x_ref.shape
    n_local, _, hidden_dim = wg_ref.shape
    n_tiles = d_model // TILE

    def expert_copies(j, slot):
        return (pltpu.make_async_copy(wg_ref.at[j], ring.at[slot, 0], ring_sem.at[slot, 0]),
                pltpu.make_async_copy(wu_ref.at[j], ring.at[slot, 1], ring_sem.at[slot, 1]))

    def shared_copies(slot):
        return (pltpu.make_async_copy(wsg_ref, ring.at[slot, 0], ring_sem.at[slot, 0]),
                pltpu.make_async_copy(wsu_ref, ring.at[slot, 1], ring_sem.at[slot, 1]))

    def down_copies(i, slot):
        cols = pl.ds(pl.multiple_of(i * TILE, TILE), TILE)
        return (pltpu.make_async_copy(wd_ref.at[:, :, cols], down.at[slot, pl.ds(0, n_local)], down_sem.at[slot, 0]),
                pltpu.make_async_copy(wsd_ref.at[:, cols], down.at[slot, n_local], down_sem.at[slot, 1]))

    def start(copies):
        for c in copies:
            c.start()

    def wait(copies):
        for c in copies:
            c.wait()

    start(expert_copies(0, 0))
    start(expert_copies(1, 1))

    barrier = pltpu.get_barrier_semaphore()
    for dev in ({'ep': mate}, {'ep': across}, {'ep': diagonal}, {'tp': 1 - tp}):
        pl.semaphore_signal(barrier, inc=1, device_id=dev, device_id_type=MESH_ID)
    pl.semaphore_wait(barrier, 4)

    def remote(src, dst, ssem, rsem, dev):
        return pltpu.make_async_remote_copy(src_ref=src, dst_ref=dst, send_sem=ssem, recv_sem=rsem, device_id=dev, device_id_type=MESH_ID)

    def gate_rows(shard):
        return gt_ref.at[pl.ds(pl.multiple_of((shard * 2 + tp) * n_local, n_local), n_local)]

    g_sends = [remote(gate_rows(peer), gates.at[ep], g_ssem.at[k], g_rsem.at[ep], {'ep': peer}) for k, peer in enumerate((mate, across, diagonal))]
    x_sends = [remote(x_ref, x_all.at[ep], x_ssem.at[k], x_rsem.at[ep], {'ep': peer}) for k, peer in enumerate((mate, across))]
    a_send = remote(attn_ref, attn_rx, a_sem.at[0], a_sem.at[1], {'tp': 1 - tp})
    start(g_sends)
    start(x_sends)
    a_send.start()

    def recv_wait(dst, sem):
        pltpu.make_async_copy(dst, dst, sem).wait()

    lane = lax.broadcasted_iota(jnp.int32, (tokens, tokens), 1)
    row = lax.broadcasted_iota(jnp.int32, (tokens, tokens), 0)
    before = (row < lane).astype(jnp.bfloat16)
    slot_row = lax.broadcasted_iota(jnp.int32, (SLOT, tokens), 0).astype(jnp.float32)

    def dispatch(s, block):
        rows = pl.ds(pl.multiple_of(s * SLOT, SLOT), SLOT)
        gate = gates[s]
        chosen = (gate > 0.0).astype(jnp.float32)
        pos = jnp.dot(chosen.astype(jnp.bfloat16), before, preferred_element_type=jnp.float32)
        for j in range(n_local):
            hit = (pos[j:j + 1, :] == slot_row) & (chosen[j:j + 1, :] > 0.0)
            place[j * SLOT:(j + 1) * SLOT, :] = jnp.where(hit, 1.0, 0.0)
            picked = jnp.sum(jnp.where(hit, gate[j:j + 1, :], 0.0), axis=-1, keepdims=True)
            slot_gate[j, rows, :] = jnp.broadcast_to(picked, (SLOT, tokens))
        placed = place[...]
        place_t[s] = placed.T.astype(jnp.bfloat16)
        placed = placed.astype(jnp.bfloat16)

        def gather(n, carry):
            cols = pl.ds(pl.multiple_of(n * TILE, TILE), TILE)
            got = jnp.dot(placed, block[:, cols], preferred_element_type=jnp.float32).astype(jnp.bfloat16)
            x_rows[:, rows, cols] = got.reshape(n_local, SLOT, TILE)
            return carry
        lax.fori_loop(0, n_tiles, gather, 0)

    gates[ep] = gt_ref[pl.ds(pl.multiple_of((ep * 2 + tp) * n_local, n_local), n_local), :]
    dispatch(ep, x_ref)
    for src in (mate, across, diagonal):
        recv_wait(gates.at[src], g_rsem.at[src])
    recv_wait(x_all.at[mate], x_rsem.at[mate])
    dispatch(mate, x_all.at[mate])
    recv_wait(x_all.at[across], x_rsem.at[across])
    x_fwd = remote(x_all.at[across], x_all.at[across], x_ssem.at[2], x_rsem.at[across], {'ep': mate})
    x_fwd.start()
    dispatch(across, x_all.at[across])
    recv_wait(x_all.at[diagonal], x_rsem.at[diagonal])
    dispatch(diagonal, x_all.at[diagonal])

    def gate_up(lhs, slot, dst):
        def part(cols):
            rows = lhs[...]
            g = jnp.dot(rows, ring[slot, 0, :, cols], preferred_element_type=jnp.float32)
            u = jnp.dot(rows, ring[slot, 1, :, cols], preferred_element_type=jnp.float32)
            act[dst, :, cols] = (jax.nn.silu(g) * u).astype(jnp.bfloat16)

        def step(n, carry):
            part(pl.ds(pl.multiple_of(n * TILE, TILE), TILE))
            return carry
        full = hidden_dim // TILE
        lax.fori_loop(0, full, step, 0)
        if hidden_dim % TILE:
            part(pl.ds(full * TILE, hidden_dim - full * TILE))

    def expert(j, carry):
        slot = j % 2
        wait(expert_copies(j, slot))
        gate_up(x_rows.at[j], slot, j)

        @pl.when(j + 2 < n_local)
        def _():
            start(expert_copies(j + 2, slot))

        @pl.when(j + 2 == n_local)
        def _():
            start(shared_copies(slot))
        return carry
    lax.fori_loop(0, n_local, expert, 0)
    shared_slot = n_local % 2
    start(down_copies(0, 0))

    recv_wait(attn_rx, a_sem.at[1])
    block_rows = 16

    def ffn_norm(r, carry):
        rows = pl.ds(pl.multiple_of(r * block_rows, block_rows), block_rows)
        attn = (attn_ref[rows, :].astype(jnp.float32) + attn_rx[rows, :].astype(jnp.float32)).astype(jnp.bfloat16).astype(jnp.float32)
        res = h_ref[rows, :].astype(jnp.float32) + attn
        attn_sum[rows, :] = res
        y_norm[rows, :] = rms_norm(res, gain_ref[...]).astype(jnp.bfloat16)
        return carry
    lax.fori_loop(0, tokens // block_rows, ffn_norm, 0)
    wait(shared_copies(shared_slot))
    gate_up(y_norm, shared_slot, n_local)
    start(down_copies(1, 1))

    def split3(v):
        a = v.astype(jnp.bfloat16)
        r = v - a.astype(jnp.float32)
        b = r.astype(jnp.bfloat16)
        c = (r - b.astype(jnp.float32)).astype(jnp.bfloat16)
        return a, b, c

    def combine(s):
        rows = pl.ds(pl.multiple_of(s * SLOT, SLOT), SLOT)
        parts = split3(y_rows[:, rows, :].reshape(n_local * SLOT, TILE))
        onehot = place_t[s]
        sums = [jnp.dot(onehot, p, preferred_element_type=jnp.float32) for p in parts]
        return sums[0] + (sums[1] + sums[2])

    def s1_copy(i):
        return remote(send1.at[i], recv1.at[i], s1_sem.at[i], r1_sem.at[i], {'ep': mate})

    def s2_copy(i):
        return remote(send2.at[i], recv2.at[i], s2_sem.at[i], r2_sem.at[i], {'ep': across})

    def s3_copy(i):
        return remote(send3.at[i], recv3.at[i], s3_sem.at[i], r3_sem.at[i], {'tp': 1 - tp})

    def down_tile(i, slot):
        wait(down_copies(i, slot))

        def one(j, carry):
            out = jnp.dot(act[j], down[slot, j], preferred_element_type=jnp.float32)
            gate = slot_gate[j]
            y_rows[j] = out * jnp.concatenate([gate] * (TILE // tokens), axis=-1)
            return carry
        lax.fori_loop(0, n_local, one, 0)
        for b in range(2):
            send1[i, b] = combine(b * 2 + 1 - core).astype(jnp.bfloat16)
        s1_copy(i).start()
        keep_other[i] = combine((1 - chip) * 2 + core)
        keep_own[i] = combine(ep) + jnp.dot(act[n_local], down[slot, n_local], preferred_element_type=jnp.float32)

        @pl.when(i + 2 < n_tiles)
        def _():
            start(down_copies(i + 2, slot))

    def step(i, carry):
        @pl.when(i < n_tiles)
        def _():
            down_tile(i, i % 2)

        @pl.when((i >= LAG1) & (i < n_tiles + LAG1))
        def _():
            k = i - LAG1
            recv_wait(recv1.at[k], r1_sem.at[k])
            send2[k] = (keep_other[k] + recv1[k, 1 - chip].astype(jnp.float32)).astype(jnp.bfloat16)
            s2_copy(k).start()
            keep_own[k] = keep_own[k] + recv1[k, chip].astype(jnp.float32)

        @pl.when((i >= LAG2) & (i < n_tiles + LAG2))
        def _():
            k = i - LAG2
            recv_wait(recv2.at[k], r2_sem.at[k])
            send3[k] = (keep_own[k] + recv2[k].astype(jnp.float32)).astype(jnp.bfloat16)
            s3_copy(k).start()

        @pl.when(i >= LAG3)
        def _():
            k = i - LAG3
            cols = pl.ds(pl.multiple_of(k * TILE, TILE), TILE)
            recv_wait(recv3.at[k], r3_sem.at[k])
            ffn = send3[k].astype(jnp.float32) + recv3[k].astype(jnp.float32)
            out_ref[:, cols] = (attn_sum[:, cols] + ffn).astype(jnp.bfloat16)
        return carry
    lax.fori_loop(0, n_tiles + LAG3, step, 0)

    for c in g_sends + x_sends + [x_fwd, a_send]:
        c.wait_send()

    def drain(i, carry):
        s1_copy(i).wait_send()
        s2_copy(i).wait_send()
        s3_copy(i).wait_send()
        return carry
    lax.fori_loop(0, n_tiles, drain, 0)


LAG1, LAG2, LAG3 = 1, 4, 7


def moe(x_norm, attn_part, hidden, gates, g_ffn, ws_gate, ws_up, ws_down, w_gate, w_up, w_down):
    tokens, d_model = x_norm.shape
    n_local, _, hidden_dim = w_gate.shape
    n_tiles = d_model // TILE
    bf16, f32 = jnp.bfloat16, jnp.float32
    dma = pltpu.SemaphoreType.DMA
    vmem = pl.BlockSpec(memory_space=pltpu.VMEM)
    hbm = pl.BlockSpec(memory_space=pltpu.HBM)
    return pl.pallas_call(
        moe_kernel,
        out_shape=jax.ShapeDtypeStruct((tokens, d_model), bf16),
        in_specs=[vmem] * 5 + [hbm] * 6,
        out_specs=vmem,
        scratch_shapes=[
            pltpu.VMEM((4, tokens, d_model), bf16),
            pltpu.VMEM((n_local, 4 * SLOT, d_model), bf16),
            pltpu.VMEM((n_local + 1, tokens, hidden_dim), bf16),
            pltpu.VMEM((4, tokens, n_local * SLOT), bf16),
            pltpu.VMEM((n_local, 4 * SLOT, tokens), f32),
            pltpu.VMEM((n_local * SLOT, tokens), f32),
            pltpu.VMEM((n_local, 4 * SLOT, TILE), f32),
            pltpu.VMEM((2, 2, d_model, hidden_dim), bf16),
            pltpu.VMEM((2, n_local + 1, hidden_dim, TILE), bf16),
            pltpu.VMEM((tokens, d_model), bf16),
            pltpu.VMEM((tokens, d_model), f32),
            pltpu.VMEM((tokens, d_model), bf16),
            pltpu.VMEM((4, n_local, tokens), f32),
            pltpu.VMEM((n_tiles, 2, tokens, TILE), bf16),
            pltpu.VMEM((n_tiles, 2, tokens, TILE), bf16),
            pltpu.VMEM((n_tiles, tokens, TILE), bf16),
            pltpu.VMEM((n_tiles, tokens, TILE), bf16),
            pltpu.VMEM((n_tiles, tokens, TILE), bf16),
            pltpu.VMEM((n_tiles, tokens, TILE), bf16),
            pltpu.VMEM((n_tiles, tokens, TILE), f32),
            pltpu.VMEM((n_tiles, tokens, TILE), f32),
            dma((2, 2)), dma((2, 2)), dma((3,)), dma((4,)), dma((3,)), dma((4,)), dma((2,)),
        ] + [dma((n_tiles,))] * 6,
        compiler_params=pltpu.CompilerParams(collective_id=0, has_side_effects=True, vmem_limit_bytes=66 * 1024 * 1024 - 2 * 1024 * 1024 - 1024 * 1024),
        cost_estimate=pl.CostEstimate(flops=2 * tokens * (n_local + 1) * 3 * d_model * hidden_dim, bytes_accessed=(n_local + 1) * 6 * d_model * hidden_dim, transcendentals=0),
        name='moe',
    )(x_norm, attn_part, hidden, gates, g_ffn.reshape(1, d_model), ws_gate, ws_up, ws_down, w_gate, w_up, w_down)


def solution(mesh):
    tok_spec = P(('rep', 'ep'), None)
    cache_spec = P(('rep', 'ep'), None, 'tp', None)
    expert_spec = P(('ep', 'tp'), None, None)
    num_shards = mesh.shape['ep'] * mesh.shape['tp']

    def layer(hidden, g_attn, w_q, w_k, w_v, w_o, k_cache, v_cache, lengths, g_ffn, ws_gate, ws_up, ws_down, w_gate, w_up, w_down, expert_ids, gate_vals):
        h_f32 = hidden.astype(jnp.float32)
        x_norm = rms_norm(h_f32, g_attn).astype(jnp.bfloat16)
        heads_out = attention_heads(x_norm, w_q, w_k, w_v, k_cache, v_cache, lengths)
        attn_part = jnp.dot(heads_out, w_o, preferred_element_type=jnp.float32).astype(jnp.bfloat16)
        gates = gate_table(expert_ids, gate_vals, w_gate.shape[0] * num_shards)
        return moe(x_norm, attn_part, hidden, gates, g_ffn, ws_gate, ws_up, ws_down, w_gate, w_up, w_down)

    in_specs = (tok_spec, P(None), P(None, 'tp'), P(None, 'tp'), P(None, 'tp'), P('tp', None), cache_spec, cache_spec, P(('rep', 'ep')), P(None), P(None, 'tp'), P(None, 'tp'), P('tp', None), expert_spec, expert_spec, expert_spec, tok_spec, tok_spec)
    return jax.shard_map(layer, mesh=mesh, in_specs=in_specs, out_specs=tok_spec, check_vma=False)
```

```python
import functools

import jax
import jax.numpy as jnp
from jax import lax
from jax.experimental import pallas as pl
from jax.experimental.pallas import tpu as pltpu
from jax.sharding import PartitionSpec as P

EPS = 1e-6
TILE = 256
SLOT = 32
HEAD = 128
KV_SLOTS = 4
KV_PAIRS = 4
LAG1, LAG2, LAG3 = 1, 4, 7
MESH_ID = pl.DeviceIdType.MESH


def rms_norm(values, gain):
    return values * lax.rsqrt(jnp.mean(values * values, axis=-1, keepdims=True) + EPS) * gain


def layer_kernel(len_ref, h_ref, gain_a_ref, gain_f_ref, ids_ref, gv_ref, wq_ref, wk_ref, wv_ref, wo_ref, kc_ref, vc_ref,
                 wsg_ref, wsu_ref, wsd_ref, wg_ref, wu_ref, wd_ref, out_ref,
                 x_all, x_rows, act, place_t, slot_gate, place, y_rows, ring, down, attn_ref, attn_rx, attn_sum, y_norm, gates, gt_ref,
                 q_buf, k_buf, v_buf, o_buf, o_rows, send1, recv1, send2, recv2, send3, recv3, keep_own, keep_other,
                 ring_sem, down_sem, kv_sem, w_sem, x_ssem, x_rsem, g_ssem, g_rsem, a_sem, s1_sem, r1_sem, s2_sem, r2_sem, s3_sem, r3_sem):
    tp = lax.axis_index('tp')
    ep = lax.axis_index('ep')
    core = ep % 2
    chip = ep // 2
    mate = chip * 2 + 1 - core
    across = (1 - chip) * 2 + core
    diagonal = (1 - chip) * 2 + 1 - core
    tokens, d_model = h_ref.shape
    n_heads = wq_ref.shape[1] // HEAD
    n_kv = wk_ref.shape[1] // HEAD
    group = n_heads // n_kv
    ctx_rows = kc_ref.shape[1] // 2
    x_ref = x_all.at[ep]
    n_local, _, hidden_dim = wg_ref.shape
    n_tiles = d_model // TILE

    def expert_copies(j, slot):
        return (pltpu.make_async_copy(wg_ref.at[j], ring.at[slot, 0], ring_sem.at[slot, 0]),
                pltpu.make_async_copy(wu_ref.at[j], ring.at[slot, 1], ring_sem.at[slot, 1]))

    def shared_copies(slot):
        return (pltpu.make_async_copy(wsg_ref, ring.at[slot, 0], ring_sem.at[slot, 0]),
                pltpu.make_async_copy(wsu_ref, ring.at[slot, 1], ring_sem.at[slot, 1]))

    def down_copies(i, slot):
        cols = pl.ds(pl.multiple_of(i * TILE, TILE), TILE)
        base = slot * (n_local + 1)
        return (pltpu.make_async_copy(wd_ref.at[:, :, cols], down.at[pl.ds(base, n_local)], down_sem.at[slot, 0]),
                pltpu.make_async_copy(wsd_ref.at[:, cols], down.at[base + n_local], down_sem.at[slot, 1]))

    def cache_copies(g):
        slot = g % KV_SLOTS
        copies = []
        for k in range(KV_PAIRS):
            dst = down.at[slot * KV_PAIRS + k, pl.ds(0, 2 * ctx_rows)]
            for n, ref in enumerate((kc_ref, vc_ref)):
                copies.append(pltpu.make_async_copy(ref.at[g * KV_PAIRS + k], dst.at[:, pl.ds(n * HEAD, HEAD)], kv_sem.at[slot, k, n]))
        return copies

    def start(copies):
        for c in copies:
            c.start()

    def wait(copies):
        for c in copies:
            c.wait()

    qw, kvw, half = n_heads * HEAD, n_kv * HEAD, d_model // 2
    proj = (pltpu.make_async_copy(wq_ref, ring.at[0, 0, :, pl.ds(0, qw)], w_sem.at[0]),
            pltpu.make_async_copy(wk_ref, ring.at[0, 1, :, pl.ds(0, kvw)], w_sem.at[1]),
            pltpu.make_async_copy(wv_ref, ring.at[0, 1, :, pl.ds(kvw, kvw)], w_sem.at[2]))
    out_proj = [pltpu.make_async_copy(wo_ref.at[:, pl.ds(b * half, half)], ring.at[1, 0, pl.ds(b * qw, qw), pl.ds(0, half)], w_sem.at[3 + b]) for b in range(2)]
    start(proj)
    for g in range(KV_SLOTS):
        start(cache_copies(g))
    start(out_proj)

    barrier = pltpu.get_barrier_semaphore()
    for dev in ({'ep': mate}, {'ep': across}, {'ep': diagonal}, {'tp': 1 - tp}):
        pl.semaphore_signal(barrier, inc=1, device_id=dev, device_id_type=MESH_ID)

    block_rows = 16
    expert_row = lax.broadcasted_iota(jnp.int32, gt_ref.shape, 0)
    table = jnp.zeros(gt_ref.shape, jnp.float32)
    for j in range(ids_ref.shape[0]):
        table = table + jnp.where(ids_ref[j:j + 1, :] == expert_row, gv_ref[j:j + 1, :], 0.0)
    gt_ref[...] = table

    def attn_norm(r, carry):
        rows = pl.ds(pl.multiple_of(r * block_rows, block_rows), block_rows)
        x_ref[rows, :] = rms_norm(h_ref[rows, :].astype(jnp.float32), gain_a_ref[...]).astype(jnp.bfloat16)
        return carry
    lax.fori_loop(0, tokens // block_rows, attn_norm, 0)

    pl.semaphore_wait(barrier, 4)

    def remote(src, dst, ssem, rsem, dev):
        return pltpu.make_async_remote_copy(src_ref=src, dst_ref=dst, send_sem=ssem, recv_sem=rsem, device_id=dev, device_id_type=MESH_ID)

    def gate_rows(shard):
        return gt_ref.at[pl.ds(pl.multiple_of((shard * 2 + tp) * n_local, n_local), n_local)]

    g_sends = [remote(gate_rows(peer), gates.at[ep], g_ssem.at[k], g_rsem.at[ep], {'ep': peer}) for k, peer in enumerate((mate, across, diagonal))]
    x_sends = [remote(x_ref, x_all.at[ep], x_ssem.at[k], x_rsem.at[ep], {'ep': peer}) for k, peer in enumerate((mate, across))]
    a_send = remote(attn_ref, attn_rx, a_sem.at[0], a_sem.at[1], {'tp': 1 - tp})
    start(g_sends)
    start(x_sends)

    def recv_wait(dst, sem):
        pltpu.make_async_copy(dst, dst, sem).wait()

    lane = lax.broadcasted_iota(jnp.int32, (tokens, tokens), 1)
    row = lax.broadcasted_iota(jnp.int32, (tokens, tokens), 0)
    before = (row < lane).astype(jnp.bfloat16)
    slot_row = lax.broadcasted_iota(jnp.int32, (SLOT, tokens), 0).astype(jnp.float32)

    def dispatch(s, block):
        rows = pl.ds(pl.multiple_of(s * SLOT, SLOT), SLOT)
        gate = gates[s]
        chosen = (gate > 0.0).astype(jnp.float32)
        pos = jnp.dot(chosen.astype(jnp.bfloat16), before, preferred_element_type=jnp.float32)
        for j in range(n_local):
            hit = (pos[j:j + 1, :] == slot_row) & (chosen[j:j + 1, :] > 0.0)
            place[j * SLOT:(j + 1) * SLOT, :] = jnp.where(hit, 1.0, 0.0)
            picked = jnp.sum(jnp.where(hit, gate[j:j + 1, :], 0.0), axis=-1, keepdims=True)
            slot_gate[j, rows, :] = jnp.broadcast_to(picked, (SLOT, tokens))
        placed = place[...]
        place_t[s] = placed.T.astype(jnp.bfloat16)
        placed = placed.astype(jnp.bfloat16)

        def gather(n, carry):
            cols = pl.ds(pl.multiple_of(n * TILE, TILE), TILE)
            got = jnp.dot(placed, block[:, cols], preferred_element_type=jnp.float32).astype(jnp.bfloat16)
            x_rows[:, rows, cols] = got.reshape(n_local, SLOT, TILE)
            return carry
        lax.fori_loop(0, n_tiles, gather, 0)

    x_own = x_ref[...]
    wait(proj)
    for n in range(qw // TILE):
        got = jnp.dot(x_own, ring[0, 0, :, n * TILE:(n + 1) * TILE], preferred_element_type=jnp.float32).astype(jnp.bfloat16).astype(jnp.float32)
        for k in range(TILE // HEAD):
            q_buf[:, n * (TILE // HEAD) + k, :] = got[:, k * HEAD:(k + 1) * HEAD]
    for n, buf in enumerate((k_buf, v_buf)):
        got = jnp.dot(x_own, ring[0, 1, :, n * kvw:(n + 1) * kvw], preferred_element_type=jnp.float32).astype(jnp.bfloat16).astype(jnp.float32)
        for k in range(n_heads):
            buf[:, k, :] = got[:, (k // group) * HEAD:(k // group + 1) * HEAD]
    start(expert_copies(0, 0))

    scale = HEAD ** -0.5
    cache_lane = lax.broadcasted_iota(jnp.int32, (n_heads, ctx_rows), 1)
    head_row = lax.broadcasted_iota(jnp.int32, (n_heads, ctx_rows), 0)
    cache_pos = jnp.where(cache_lane % n_kv == head_row // group, cache_lane // n_kv, ctx_rows)

    def attend(g, carry):
        wait(cache_copies(g))
        base = (g % KV_SLOTS) * KV_PAIRS
        for u in range(2 * KV_PAIRS):
            t = g * (2 * KV_PAIRS) + u
            rows = slice((u % 2) * ctx_rows, (u % 2 + 1) * ctx_rows)
            unit = base + u // 2
            q = q_buf[t]
            s = lax.dot_general(q.astype(jnp.bfloat16), down[unit, rows, 0:HEAD], (((1,), (1,)), ((), ())), preferred_element_type=jnp.float32) * scale
            s = jnp.where(cache_pos < len_ref[t], s, -jnp.inf)
            own = jnp.sum(q * k_buf[t], axis=-1, keepdims=True) * scale
            top = jnp.maximum(jnp.max(s, axis=-1, keepdims=True), own)
            w = jnp.exp(s - top)
            w_own = jnp.exp(own - top)
            norm = jnp.sum(w, axis=-1, keepdims=True) + w_own
            mixed = jnp.dot(w.astype(jnp.bfloat16), down[unit, rows, HEAD:2 * HEAD], preferred_element_type=jnp.float32)
            o_buf[t] = (mixed + w_own.astype(jnp.bfloat16).astype(jnp.float32) * v_buf[t]) / norm

        @pl.when(g + KV_SLOTS < tokens // (2 * KV_PAIRS))
        def _():
            start(cache_copies(g + KV_SLOTS))
        return carry
    lax.fori_loop(0, tokens // (2 * KV_PAIRS), attend, 0)

    recv_wait(x_all.at[across], x_rsem.at[across])
    x_fwd = remote(x_all.at[across], x_all.at[across], x_ssem.at[2], x_rsem.at[across], {'ep': mate})
    x_fwd.start()

    for k in range(n_heads):
        o_rows[:, k * HEAD:(k + 1) * HEAD] = o_buf[:, k, :].astype(jnp.bfloat16)
    wait(out_proj)
    for b in range(2):
        def project(n, carry, b=b):
            cols = pl.ds(pl.multiple_of(n * TILE, TILE), TILE)
            got = jnp.dot(o_rows[...], ring[1, 0, pl.ds(b * qw, qw), cols], preferred_element_type=jnp.float32)
            attn_ref[:, pl.ds(pl.multiple_of(b * half + n * TILE, TILE), TILE)] = got.astype(jnp.bfloat16)
            return carry
        lax.fori_loop(0, half // TILE, project, 0)
    start(expert_copies(1, 1))

    gates[ep] = gt_ref[pl.ds(pl.multiple_of((ep * 2 + tp) * n_local, n_local), n_local), :]
    dispatch(ep, x_ref)
    for src in (mate, across, diagonal):
        recv_wait(gates.at[src], g_rsem.at[src])
    recv_wait(x_all.at[mate], x_rsem.at[mate])
    dispatch(mate, x_all.at[mate])
    a_send.start()
    dispatch(across, x_all.at[across])
    recv_wait(x_all.at[diagonal], x_rsem.at[diagonal])
    dispatch(diagonal, x_all.at[diagonal])

    def gate_up(lhs, slot, dst):
        def part(cols):
            rows = lhs[...]
            g = jnp.dot(rows, ring[slot, 0, :, cols], preferred_element_type=jnp.float32)
            u = jnp.dot(rows, ring[slot, 1, :, cols], preferred_element_type=jnp.float32)
            act[dst, :, cols] = (jax.nn.silu(g) * u).astype(jnp.bfloat16)

        def step(n, carry):
            part(pl.ds(pl.multiple_of(n * TILE, TILE), TILE))
            return carry
        full = hidden_dim // TILE
        lax.fori_loop(0, full, step, 0)
        if hidden_dim % TILE:
            part(pl.ds(full * TILE, hidden_dim - full * TILE))

    def expert(j, carry):
        slot = j % 2
        wait(expert_copies(j, slot))
        gate_up(x_rows.at[j], slot, j)

        @pl.when(j + 2 < n_local)
        def _():
            start(expert_copies(j + 2, slot))

        @pl.when(j + 2 == n_local)
        def _():
            start(shared_copies(slot))
        return carry
    lax.fori_loop(0, n_local, expert, 0)
    shared_slot = n_local % 2
    start(down_copies(0, 0))

    recv_wait(attn_rx, a_sem.at[1])

    def ffn_norm(r, carry):
        rows = pl.ds(pl.multiple_of(r * block_rows, block_rows), block_rows)
        attn = (attn_ref[rows, :].astype(jnp.float32) + attn_rx[rows, :].astype(jnp.float32)).astype(jnp.bfloat16).astype(jnp.float32)
        res = h_ref[rows, :].astype(jnp.float32) + attn
        attn_sum[rows, :] = res
        y_norm[rows, :] = rms_norm(res, gain_f_ref[...]).astype(jnp.bfloat16)
        return carry
    lax.fori_loop(0, tokens // block_rows, ffn_norm, 0)
    wait(shared_copies(shared_slot))
    gate_up(y_norm, shared_slot, n_local)
    start(down_copies(1, 1))

    def split3(v):
        a = v.astype(jnp.bfloat16)
        r = v - a.astype(jnp.float32)
        b = r.astype(jnp.bfloat16)
        c = (r - b.astype(jnp.float32)).astype(jnp.bfloat16)
        return a, b, c

    def combine(s):
        rows = pl.ds(pl.multiple_of(s * SLOT, SLOT), SLOT)
        parts = split3(y_rows[:, rows, :].reshape(n_local * SLOT, TILE))
        onehot = place_t[s]
        sums = [jnp.dot(onehot, p, preferred_element_type=jnp.float32) for p in parts]
        return sums[0] + (sums[1] + sums[2])

    def s1_copy(i):
        return remote(send1.at[i], recv1.at[i], s1_sem.at[i], r1_sem.at[i], {'ep': mate})

    def s2_copy(i):
        return remote(send2.at[i], recv2.at[i], s2_sem.at[i], r2_sem.at[i], {'ep': across})

    def s3_copy(i):
        return remote(send3.at[i], recv3.at[i], s3_sem.at[i], r3_sem.at[i], {'tp': 1 - tp})

    def down_tile(i, slot):
        wait(down_copies(i, slot))

        def one(j, carry):
            out = jnp.dot(act[j], down[slot * (n_local + 1) + j], preferred_element_type=jnp.float32)
            gate = slot_gate[j]
            y_rows[j] = out * jnp.concatenate([gate] * (TILE // tokens), axis=-1)
            return carry
        lax.fori_loop(0, n_local, one, 0)
        for b in range(2):
            send1[i, b] = combine(b * 2 + 1 - core).astype(jnp.bfloat16)
        s1_copy(i).start()
        keep_other[i] = combine((1 - chip) * 2 + core)
        keep_own[i] = combine(ep) + jnp.dot(act[n_local], down[slot * (n_local + 1) + n_local], preferred_element_type=jnp.float32)

        @pl.when(i + 2 < n_tiles)
        def _():
            start(down_copies(i + 2, slot))

    def step(i, carry):
        @pl.when(i < n_tiles)
        def _():
            down_tile(i, i % 2)

        @pl.when((i >= LAG1) & (i < n_tiles + LAG1))
        def _():
            k = i - LAG1
            recv_wait(recv1.at[k], r1_sem.at[k])
            send2[k] = (keep_other[k] + recv1[k, 1 - chip].astype(jnp.float32)).astype(jnp.bfloat16)
            s2_copy(k).start()
            keep_own[k] = keep_own[k] + recv1[k, chip].astype(jnp.float32)

        @pl.when((i >= LAG2) & (i < n_tiles + LAG2))
        def _():
            k = i - LAG2
            recv_wait(recv2.at[k], r2_sem.at[k])
            send3[k] = (keep_own[k] + recv2[k].astype(jnp.float32)).astype(jnp.bfloat16)
            s3_copy(k).start()

        @pl.when(i >= LAG3)
        def _():
            k = i - LAG3
            cols = pl.ds(pl.multiple_of(k * TILE, TILE), TILE)
            recv_wait(recv3.at[k], r3_sem.at[k])
            ffn = send3[k].astype(jnp.float32) + recv3[k].astype(jnp.float32)
            out_ref[:, cols] = (attn_sum[:, cols] + ffn).astype(jnp.bfloat16)
        return carry
    lax.fori_loop(0, n_tiles + LAG3, step, 0)

    for c in g_sends + x_sends + [x_fwd, a_send]:
        c.wait_send()

    def drain(i, carry):
        s1_copy(i).wait_send()
        s2_copy(i).wait_send()
        s3_copy(i).wait_send()
        return carry
    lax.fori_loop(0, n_tiles, drain, 0)


def fused_layer(hidden, g_attn, w_q, w_k, w_v, w_o, k_cache, v_cache, lengths, g_ffn, ws_gate, ws_up, ws_down, w_gate, w_up, w_down, expert_ids, gate_vals, shards):
    tokens, d_model = hidden.shape
    n_local, _, hidden_dim = w_gate.shape
    n_tiles = d_model // TILE
    n_heads = w_q.shape[1] // HEAD
    ctx_len, n_kv = k_cache.shape[1:3]
    bf16, f32 = jnp.bfloat16, jnp.float32
    dma = pltpu.SemaphoreType.DMA
    vmem = pl.BlockSpec(memory_space=pltpu.VMEM)
    hbm = pl.BlockSpec(memory_space=pltpu.HBM)
    smem = pl.BlockSpec(memory_space=pltpu.SMEM)
    tile = pltpu.VMEM((n_tiles, tokens, TILE), bf16)
    tile_f32 = pltpu.VMEM((n_tiles, tokens, TILE), f32)
    pair_tile = pltpu.VMEM((n_tiles, 2, tokens, TILE), bf16)
    rows_bf16 = pltpu.VMEM((tokens, d_model), bf16)
    heads = pltpu.VMEM((tokens, n_heads, HEAD), f32)
    caches = [c.reshape(tokens // 2, 2 * ctx_len * n_kv, HEAD) for c in (k_cache, v_cache)]
    return pl.pallas_call(
        layer_kernel,
        out_shape=jax.ShapeDtypeStruct((tokens, d_model), bf16),
        in_specs=[smem] + [vmem] * 5 + [hbm] * 12,
        out_specs=vmem,
        scratch_shapes=[
            pltpu.VMEM((4, tokens, d_model), bf16),
            pltpu.VMEM((n_local, 4 * SLOT, d_model), bf16),
            pltpu.VMEM((n_local + 1, tokens, hidden_dim), bf16),
            pltpu.VMEM((4, tokens, n_local * SLOT), bf16),
            pltpu.VMEM((n_local, 4 * SLOT, tokens), f32),
            pltpu.VMEM((n_local * SLOT, tokens), f32),
            pltpu.VMEM((n_local, 4 * SLOT, TILE), f32),
            pltpu.VMEM((2, 2, d_model, hidden_dim), bf16),
            pltpu.VMEM((2 * (n_local + 1), hidden_dim, TILE), bf16),
            rows_bf16, rows_bf16,
            pltpu.VMEM((tokens, d_model), f32),
            rows_bf16,
            pltpu.VMEM((4, n_local, tokens), f32),
            pltpu.VMEM((n_local * shards, tokens), f32),
            heads, heads, heads, heads,
            pltpu.VMEM((tokens, n_heads * HEAD), bf16),
            pair_tile, pair_tile, tile, tile, tile, tile, tile_f32, tile_f32,
            dma((2, 2)), dma((2, 2)), dma((KV_SLOTS, KV_PAIRS, 2)), dma((5,)), dma((3,)), dma((4,)), dma((3,)), dma((4,)), dma((2,)),
        ] + [dma((n_tiles,))] * 6,
        compiler_params=pltpu.CompilerParams(collective_id=0, has_side_effects=True, vmem_limit_bytes=63 * 1024 * 1024),
        cost_estimate=pl.CostEstimate(flops=2 * tokens * (n_local + 1) * 3 * d_model * hidden_dim, bytes_accessed=(n_local + 1) * 6 * d_model * hidden_dim, transcendentals=0),
        name='layer',
    )(lengths, hidden, g_attn.reshape(1, d_model), g_ffn.reshape(1, d_model), expert_ids.T, gate_vals.T, w_q, w_k, w_v, w_o, *caches, ws_gate, ws_up, ws_down, w_gate, w_up, w_down)


def solution(mesh):
    tok_spec = P(('rep', 'ep'), None)
    cache_spec = P(('rep', 'ep'), None, 'tp', None)
    expert_spec = P(('ep', 'tp'), None, None)
    layer = functools.partial(fused_layer, shards=mesh.shape['ep'] * mesh.shape['tp'])
    in_specs = (tok_spec, P(None), P(None, 'tp'), P(None, 'tp'), P(None, 'tp'), P('tp', None), cache_spec, cache_spec, P(('rep', 'ep')), P(None), P(None, 'tp'), P(None, 'tp'), P('tp', None), expert_spec, expert_spec, expert_spec, tok_spec, tok_spec)
    return jax.shard_map(layer, mesh=mesh, in_specs=in_specs, out_specs=tok_spec, check_vma=False)
```

```python
import functools

import jax
import jax.numpy as jnp
from jax import lax
from jax.experimental import pallas as pl
from jax.experimental.pallas import tpu as pltpu
from jax.sharding import PartitionSpec as P

EPS = 1e-6
TILE = 256
SLOT = 32
HEAD = 128
KV_SLOTS = 4
KV_PAIRS = 4
LAG1, LAG2, LAG3 = 1, 4, 7
MESH_ID = pl.DeviceIdType.MESH


def rms_norm(values, gain):
    return values * lax.rsqrt(jnp.mean(values * values, axis=-1, keepdims=True) + EPS) * gain


def layer_kernel(len_ref, h_ref, gain_a_ref, gain_f_ref, ids_ref, gv_ref, wq_ref, wk_ref, wv_ref, wo_ref, kc_ref, vc_ref,
                 wsg_ref, wsu_ref, wsd_ref, wg_ref, wu_ref, wd_ref, out_ref,
                 x_all, x_rows, act, place_t, slot_gate, place, y_parts, ring, down, attn_ref, attn_rx, attn_sum, y_norm, gates, gt_ref,
                 q_buf, k_buf, v_buf, o_buf, o_rows, send1, recv1, send2, recv2, send3, recv3, keep_own, keep_other,
                 ring_sem, down_sem, kv_sem, w_sem, x_ssem, x_rsem, g_ssem, g_rsem, a_sem, s1_sem, r1_sem, s2_sem, r2_sem, s3_sem, r3_sem):
    tp = lax.axis_index('tp')
    ep = lax.axis_index('ep')
    core = ep % 2
    chip = ep // 2
    mate = chip * 2 + 1 - core
    across = (1 - chip) * 2 + core
    diagonal = (1 - chip) * 2 + 1 - core
    tokens, d_model = h_ref.shape
    n_heads = wq_ref.shape[1] // HEAD
    n_kv = wk_ref.shape[1] // HEAD
    group = n_heads // n_kv
    ctx_rows = kc_ref.shape[1] // 2
    x_ref = x_all.at[ep]
    n_local, _, hidden_dim = wg_ref.shape
    n_tiles = d_model // TILE

    def expert_copies(j, slot):
        return (pltpu.make_async_copy(wg_ref.at[j], ring.at[slot, 0], ring_sem.at[slot, 0]),
                pltpu.make_async_copy(wu_ref.at[j], ring.at[slot, 1], ring_sem.at[slot, 1]))

    def shared_copies(slot):
        return (pltpu.make_async_copy(wsg_ref, ring.at[slot, 0], ring_sem.at[slot, 0]),
                pltpu.make_async_copy(wsu_ref, ring.at[slot, 1], ring_sem.at[slot, 1]))

    def down_copies(i, slot):
        cols = pl.ds(pl.multiple_of(i * TILE, TILE), TILE)
        base = slot * (n_local + 1)
        return (pltpu.make_async_copy(wd_ref.at[:, :, cols], down.at[pl.ds(base, n_local)], down_sem.at[slot, 0]),
                pltpu.make_async_copy(wsd_ref.at[:, cols], down.at[base + n_local], down_sem.at[slot, 1]))

    def cache_copies(g):
        slot = g % KV_SLOTS
        copies = []
        for k in range(KV_PAIRS):
            dst = down.at[slot * KV_PAIRS + k, pl.ds(0, 2 * ctx_rows)]
            for n, ref in enumerate((kc_ref, vc_ref)):
                copies.append(pltpu.make_async_copy(ref.at[g * KV_PAIRS + k], dst.at[:, pl.ds(n * HEAD, HEAD)], kv_sem.at[slot, k, n]))
        return copies

    def start(copies):
        for c in copies:
            c.start()

    def wait(copies):
        for c in copies:
            c.wait()

    qw, kvw, half = n_heads * HEAD, n_kv * HEAD, d_model // 2
    proj = (pltpu.make_async_copy(wq_ref, ring.at[0, 0, :, pl.ds(0, qw)], w_sem.at[0]),
            pltpu.make_async_copy(wk_ref, ring.at[0, 1, :, pl.ds(0, kvw)], w_sem.at[1]),
            pltpu.make_async_copy(wv_ref, ring.at[0, 1, :, pl.ds(kvw, kvw)], w_sem.at[2]))
    out_proj = [pltpu.make_async_copy(wo_ref.at[:, pl.ds(b * half, half)], ring.at[1, 0, pl.ds(b * qw, qw), pl.ds(0, half)], w_sem.at[3 + b]) for b in range(2)]
    start(proj)
    for g in range(KV_SLOTS):
        start(cache_copies(g))
    start(out_proj)

    barrier = pltpu.get_barrier_semaphore()
    for dev in ({'ep': mate}, {'ep': across}, {'ep': diagonal}, {'tp': 1 - tp}):
        pl.semaphore_signal(barrier, inc=1, device_id=dev, device_id_type=MESH_ID)

    block_rows = 16
    expert_row = lax.broadcasted_iota(jnp.int32, gt_ref.shape, 0)
    table = jnp.zeros(gt_ref.shape, jnp.float32)
    for j in range(ids_ref.shape[0]):
        table = table + jnp.where(ids_ref[j:j + 1, :] == expert_row, gv_ref[j:j + 1, :], 0.0)
    gt_ref[...] = table

    def attn_norm(r, carry):
        rows = pl.ds(pl.multiple_of(r * block_rows, block_rows), block_rows)
        x_ref[rows, :] = rms_norm(h_ref[rows, :].astype(jnp.float32), gain_a_ref[...]).astype(jnp.bfloat16)
        return carry
    lax.fori_loop(0, tokens // block_rows, attn_norm, 0)

    pl.semaphore_wait(barrier, 4)

    def remote(src, dst, ssem, rsem, dev):
        return pltpu.make_async_remote_copy(src_ref=src, dst_ref=dst, send_sem=ssem, recv_sem=rsem, device_id=dev, device_id_type=MESH_ID)

    def gate_rows(shard):
        return gt_ref.at[pl.ds(pl.multiple_of((shard * 2 + tp) * n_local, n_local), n_local)]

    g_sends = [remote(gate_rows(peer), gates.at[ep], g_ssem.at[k], g_rsem.at[ep], {'ep': peer}) for k, peer in enumerate((mate, across, diagonal))]
    x_sends = [remote(x_ref, x_all.at[ep], x_ssem.at[k], x_rsem.at[ep], {'ep': peer}) for k, peer in enumerate((mate, across))]
    a_send = remote(attn_ref, attn_rx, a_sem.at[0], a_sem.at[1], {'tp': 1 - tp})
    start(g_sends)
    start(x_sends)

    def recv_wait(dst, sem):
        pltpu.make_async_copy(dst, dst, sem).wait()

    lane = lax.broadcasted_iota(jnp.int32, (tokens, tokens), 1)
    row = lax.broadcasted_iota(jnp.int32, (tokens, tokens), 0)
    before = (row < lane).astype(jnp.bfloat16)
    slot_row = lax.broadcasted_iota(jnp.int32, (SLOT, tokens), 0).astype(jnp.float32)

    def dispatch(s, block):
        rows = pl.ds(pl.multiple_of(s * SLOT, SLOT), SLOT)
        gate = gates[s]
        chosen = (gate > 0.0).astype(jnp.float32)
        pos = jnp.dot(chosen.astype(jnp.bfloat16), before, preferred_element_type=jnp.float32)
        for j in range(n_local):
            hit = (pos[j:j + 1, :] == slot_row) & (chosen[j:j + 1, :] > 0.0)
            place[j * SLOT:(j + 1) * SLOT, :] = jnp.where(hit, 1.0, 0.0)
            picked = jnp.sum(jnp.where(hit, gate[j:j + 1, :], 0.0), axis=-1, keepdims=True)
            slot_gate[j, rows, :] = jnp.broadcast_to(picked, (SLOT, tokens))
        placed = place[...]
        place_t[s] = placed.T.astype(jnp.bfloat16)
        placed = placed.astype(jnp.bfloat16)

        for n in range(n_tiles):
            cols = slice(n * TILE, (n + 1) * TILE)
            got = jnp.dot(placed, block[:, cols], preferred_element_type=jnp.float32).astype(jnp.bfloat16)
            x_rows[:, rows, cols] = got.reshape(n_local, SLOT, TILE)

    x_own = x_ref[...]
    wait(proj)
    for n in range(qw // TILE):
        got = jnp.dot(x_own, ring[0, 0, :, n * TILE:(n + 1) * TILE], preferred_element_type=jnp.float32).astype(jnp.bfloat16).astype(jnp.float32)
        for k in range(TILE // HEAD):
            q_buf[:, n * (TILE // HEAD) + k, :] = got[:, k * HEAD:(k + 1) * HEAD]
    for n, buf in enumerate((k_buf, v_buf)):
        got = jnp.dot(x_own, ring[0, 1, :, n * kvw:(n + 1) * kvw], preferred_element_type=jnp.float32).astype(jnp.bfloat16).astype(jnp.float32)
        for k in range(n_heads):
            buf[:, k, :] = got[:, (k // group) * HEAD:(k // group + 1) * HEAD]
    start(expert_copies(0, 0))

    scale = HEAD ** -0.5
    cache_lane = lax.broadcasted_iota(jnp.int32, (n_heads, ctx_rows), 1)
    head_row = lax.broadcasted_iota(jnp.int32, (n_heads, ctx_rows), 0)
    cache_pos = jnp.where(cache_lane % n_kv == head_row // group, cache_lane // n_kv, ctx_rows)

    def attend(g, carry):
        wait(cache_copies(g))
        base = (g % KV_SLOTS) * KV_PAIRS
        for u in range(2 * KV_PAIRS):
            t = g * (2 * KV_PAIRS) + u
            rows = slice((u % 2) * ctx_rows, (u % 2 + 1) * ctx_rows)
            unit = base + u // 2
            q = q_buf[t]
            s = lax.dot_general(q.astype(jnp.bfloat16), down[unit, rows, 0:HEAD], (((1,), (1,)), ((), ())), preferred_element_type=jnp.float32) * scale
            s = jnp.where(cache_pos < len_ref[t], s, -jnp.inf)
            own = jnp.sum(q * k_buf[t], axis=-1, keepdims=True) * scale
            top = jnp.maximum(jnp.max(s, axis=-1, keepdims=True), own)
            w = jnp.exp(s - top)
            w_own = jnp.exp(own - top)
            norm = jnp.sum(w, axis=-1, keepdims=True) + w_own
            mixed = jnp.dot(w.astype(jnp.bfloat16), down[unit, rows, HEAD:2 * HEAD], preferred_element_type=jnp.float32)
            o_buf[t] = (mixed + w_own.astype(jnp.bfloat16).astype(jnp.float32) * v_buf[t]) / norm

        @pl.when(g + KV_SLOTS < tokens // (2 * KV_PAIRS))
        def _():
            start(cache_copies(g + KV_SLOTS))
        return carry
    lax.fori_loop(0, tokens // (2 * KV_PAIRS), attend, 0)

    recv_wait(x_all.at[across], x_rsem.at[across])
    x_fwd = remote(x_all.at[across], x_all.at[across], x_ssem.at[2], x_rsem.at[across], {'ep': mate})
    x_fwd.start()

    for k in range(n_heads):
        o_rows[:, k * HEAD:(k + 1) * HEAD] = o_buf[:, k, :].astype(jnp.bfloat16)
    wait(out_proj)
    for b in range(2):
        for n in range(half // TILE):
            got = jnp.dot(o_rows[...], ring[1, 0, b * qw:(b + 1) * qw, n * TILE:(n + 1) * TILE], preferred_element_type=jnp.float32)
            attn_ref[:, b * half + n * TILE:b * half + (n + 1) * TILE] = got.astype(jnp.bfloat16)
    start(expert_copies(1, 1))

    gates[ep] = gt_ref[pl.ds(pl.multiple_of((ep * 2 + tp) * n_local, n_local), n_local), :]
    dispatch(ep, x_ref)
    for src in (mate, across, diagonal):
        recv_wait(gates.at[src], g_rsem.at[src])
    recv_wait(x_all.at[mate], x_rsem.at[mate])
    dispatch(mate, x_all.at[mate])
    a_send.start()
    dispatch(across, x_all.at[across])
    recv_wait(x_all.at[diagonal], x_rsem.at[diagonal])
    dispatch(diagonal, x_all.at[diagonal])

    def gate_up(lhs, slot, dst):
        full = hidden_dim // TILE * TILE
        for c in range(0, full, TILE):
            cols = slice(c, c + TILE)
            g = jnp.dot(lhs[...], ring[slot, 0, :, cols], preferred_element_type=jnp.float32)
            u = jnp.dot(lhs[...], ring[slot, 1, :, cols], preferred_element_type=jnp.float32)
            act[dst, :, cols] = (jax.nn.silu(g) * u).astype(jnp.bfloat16)
        if full < hidden_dim:
            cols = slice(full, hidden_dim)
            both = jnp.concatenate([ring[slot, 0, :, cols], ring[slot, 1, :, cols]], axis=1)
            gu = jnp.dot(lhs[...], both, preferred_element_type=jnp.float32)
            rest = hidden_dim - full
            act[dst, :, cols] = (jax.nn.silu(gu[:, :rest]) * gu[:, rest:]).astype(jnp.bfloat16)

    def expert(j, carry):
        slot = j % 2
        wait(expert_copies(j, slot))
        gate_up(x_rows.at[j], slot, j)

        @pl.when(j + 2 < n_local)
        def _():
            start(expert_copies(j + 2, slot))

        @pl.when(j + 2 == n_local)
        def _():
            start(shared_copies(slot))
        return carry
    lax.fori_loop(0, n_local, expert, 0)
    shared_slot = n_local % 2
    start(down_copies(0, 0))

    recv_wait(attn_rx, a_sem.at[1])

    def ffn_norm(r, carry):
        rows = pl.ds(pl.multiple_of(r * block_rows, block_rows), block_rows)
        attn = (attn_ref[rows, :].astype(jnp.float32) + attn_rx[rows, :].astype(jnp.float32)).astype(jnp.bfloat16).astype(jnp.float32)
        res = h_ref[rows, :].astype(jnp.float32) + attn
        attn_sum[rows, :] = res
        y_norm[rows, :] = rms_norm(res, gain_f_ref[...]).astype(jnp.bfloat16)
        return carry
    lax.fori_loop(0, tokens // block_rows, ffn_norm, 0)
    wait(shared_copies(shared_slot))
    gate_up(y_norm, shared_slot, n_local)
    start(down_copies(1, 1))

    def split3(v):
        a = v.astype(jnp.bfloat16)
        r = v - a.astype(jnp.float32)
        b = r.astype(jnp.bfloat16)
        c = (r - b.astype(jnp.float32)).astype(jnp.bfloat16)
        return a, b, c

    def combine(s):
        rows = pl.ds(pl.multiple_of(s * SLOT, SLOT), SLOT)
        sums = [jnp.dot(place_t[s], y_parts[p, :, rows, :].reshape(n_local * SLOT, TILE), preferred_element_type=jnp.float32) for p in range(3)]
        return sums[0] + (sums[1] + sums[2])

    def s1_copy(i):
        return remote(send1.at[i], recv1.at[i], s1_sem.at[i], r1_sem.at[i], {'ep': mate})

    def s2_copy(i):
        return remote(send2.at[i], recv2.at[i], s2_sem.at[i], r2_sem.at[i], {'ep': across})

    def s3_copy(i):
        return remote(send3.at[i], recv3.at[i], s3_sem.at[i], r3_sem.at[i], {'tp': 1 - tp})

    def down_tile(i, slot):
        wait(down_copies(i, slot))

        for j in range(n_local):
            out = jnp.dot(act[j], down[slot * (n_local + 1) + j], preferred_element_type=jnp.float32)
            gate = slot_gate[j]
            parts = split3(out * jnp.concatenate([gate] * (TILE // tokens), axis=-1))
            for p in range(3):
                y_parts[p, j] = parts[p]
        for b in range(2):
            send1[i, b] = combine(b * 2 + 1 - core).astype(jnp.bfloat16)
        s1_copy(i).start()
        keep_other[i] = combine((1 - chip) * 2 + core)
        keep_own[i] = combine(ep) + jnp.dot(act[n_local], down[slot * (n_local + 1) + n_local], preferred_element_type=jnp.float32)

        @pl.when(i + 2 < n_tiles)
        def _():
            start(down_copies(i + 2, slot))

    def step(i, carry):
        @pl.when(i < n_tiles)
        def _():
            down_tile(i, i % 2)

        @pl.when((i >= LAG1) & (i < n_tiles + LAG1))
        def _():
            k = i - LAG1
            recv_wait(recv1.at[k], r1_sem.at[k])
            send2[k] = (keep_other[k] + recv1[k, 1 - chip].astype(jnp.float32)).astype(jnp.bfloat16)
            s2_copy(k).start()
            keep_own[k] = keep_own[k] + recv1[k, chip].astype(jnp.float32)

        @pl.when((i >= LAG2) & (i < n_tiles + LAG2))
        def _():
            k = i - LAG2
            recv_wait(recv2.at[k], r2_sem.at[k])
            send3[k] = (keep_own[k] + recv2[k].astype(jnp.float32)).astype(jnp.bfloat16)
            s3_copy(k).start()

        @pl.when(i >= LAG3)
        def _():
            k = i - LAG3
            cols = pl.ds(pl.multiple_of(k * TILE, TILE), TILE)
            recv_wait(recv3.at[k], r3_sem.at[k])
            ffn = send3[k].astype(jnp.float32) + recv3[k].astype(jnp.float32)
            out_ref[:, cols] = (attn_sum[:, cols] + ffn).astype(jnp.bfloat16)
        return carry
    lax.fori_loop(0, n_tiles + LAG3, step, 0)

    for c in g_sends + x_sends + [x_fwd, a_send]:
        c.wait_send()

    def drain(i, carry):
        s1_copy(i).wait_send()
        s2_copy(i).wait_send()
        s3_copy(i).wait_send()
        return carry
    lax.fori_loop(0, n_tiles, drain, 0)


def fused_layer(hidden, g_attn, w_q, w_k, w_v, w_o, k_cache, v_cache, lengths, g_ffn, ws_gate, ws_up, ws_down, w_gate, w_up, w_down, expert_ids, gate_vals, shards):
    tokens, d_model = hidden.shape
    n_local, _, hidden_dim = w_gate.shape
    n_tiles = d_model // TILE
    n_heads = w_q.shape[1] // HEAD
    ctx_len, n_kv = k_cache.shape[1:3]
    bf16, f32 = jnp.bfloat16, jnp.float32
    dma = pltpu.SemaphoreType.DMA
    vmem = pl.BlockSpec(memory_space=pltpu.VMEM)
    hbm = pl.BlockSpec(memory_space=pltpu.HBM)
    smem = pl.BlockSpec(memory_space=pltpu.SMEM)
    tile = pltpu.VMEM((n_tiles, tokens, TILE), bf16)
    tile_f32 = pltpu.VMEM((n_tiles, tokens, TILE), f32)
    pair_tile = pltpu.VMEM((n_tiles, 2, tokens, TILE), bf16)
    rows_bf16 = pltpu.VMEM((tokens, d_model), bf16)
    heads = pltpu.VMEM((tokens, n_heads, HEAD), f32)
    caches = [c.reshape(tokens // 2, 2 * ctx_len * n_kv, HEAD) for c in (k_cache, v_cache)]
    return pl.pallas_call(
        layer_kernel,
        out_shape=jax.ShapeDtypeStruct((tokens, d_model), bf16),
        in_specs=[smem] + [vmem] * 5 + [hbm] * 12,
        out_specs=vmem,
        scratch_shapes=[
            pltpu.VMEM((4, tokens, d_model), bf16),
            pltpu.VMEM((n_local, 4 * SLOT, d_model), bf16),
            pltpu.VMEM((n_local + 1, tokens, hidden_dim), bf16),
            pltpu.VMEM((4, tokens, n_local * SLOT), bf16),
            pltpu.VMEM((n_local, 4 * SLOT, tokens), f32),
            pltpu.VMEM((n_local * SLOT, tokens), f32),
            pltpu.VMEM((3, n_local, 4 * SLOT, TILE), bf16),
            pltpu.VMEM((2, 2, d_model, hidden_dim), bf16),
            pltpu.VMEM((2 * (n_local + 1), hidden_dim, TILE), bf16),
            rows_bf16, rows_bf16,
            pltpu.VMEM((tokens, d_model), f32),
            rows_bf16,
            pltpu.VMEM((4, n_local, tokens), f32),
            pltpu.VMEM((n_local * shards, tokens), f32),
            heads, heads, heads, heads,
            pltpu.VMEM((tokens, n_heads * HEAD), bf16),
            pair_tile, pair_tile, tile, tile, tile, tile, tile_f32, tile_f32,
            dma((2, 2)), dma((2, 2)), dma((KV_SLOTS, KV_PAIRS, 2)), dma((5,)), dma((3,)), dma((4,)), dma((3,)), dma((4,)), dma((2,)),
        ] + [dma((n_tiles,))] * 6,
        compiler_params=pltpu.CompilerParams(collective_id=0, has_side_effects=True, vmem_limit_bytes=63 * 1024 * 1024),
        cost_estimate=pl.CostEstimate(flops=2 * tokens * (n_local + 1) * 3 * d_model * hidden_dim, bytes_accessed=(n_local + 1) * 6 * d_model * hidden_dim, transcendentals=0),
        name='layer',
    )(lengths, hidden, g_attn.reshape(1, d_model), g_ffn.reshape(1, d_model), expert_ids.T, gate_vals.T, w_q, w_k, w_v, w_o, *caches, ws_gate, ws_up, ws_down, w_gate, w_up, w_down)


def solution(mesh):
    tok_spec = P(('rep', 'ep'), None)
    cache_spec = P(('rep', 'ep'), None, 'tp', None)
    expert_spec = P(('ep', 'tp'), None, None)
    layer = functools.partial(fused_layer, shards=mesh.shape['ep'] * mesh.shape['tp'])
    in_specs = (tok_spec, P(None), P(None, 'tp'), P(None, 'tp'), P(None, 'tp'), P('tp', None), cache_spec, cache_spec, P(('rep', 'ep')), P(None), P(None, 'tp'), P(None, 'tp'), P('tp', None), expert_spec, expert_spec, expert_spec, tok_spec, tok_spec)
    return jax.shard_map(layer, mesh=mesh, in_specs=in_specs, out_specs=tok_spec, check_vma=False)
```

```python
import functools

import jax
import jax.numpy as jnp
from jax import lax
from jax.experimental import pallas as pl
from jax.experimental.pallas import tpu as pltpu
from jax.sharding import PartitionSpec as P

EPS = 1e-6
TILE = 256
SLOT = 32
HEAD = 128
KV_SLOTS = 4
KV_PAIRS = 4
BATCH = 4 * KV_PAIRS
LAG1, LAG2, LAG3 = 1, 4, 7
MESH_ID = pl.DeviceIdType.MESH


def rms_norm(values, gain):
    return values * lax.rsqrt(jnp.mean(values * values, axis=-1, keepdims=True) + EPS) * gain


def layer_kernel(len_in, h_in, gain_a_in, gain_f_in, ids_in, gv_in, wq_ref, wk_ref, wv_ref, wo_ref, kc_ref, vc_ref,
                 wsg_ref, wsu_ref, wsd_ref, wg_ref, wu_ref, wd_ref, out_ref,
                 x_all, x_rows, act, place_t, slot_gate, place, y_parts, ring, down, attn_ref, attn_rx, attn_sum, y_norm, gates, gt_ref,
                 len_ref, h_ref, gain_a_ref, gain_f_ref, ids_ref, gv_ref, out_buf, q_buf, k_buf, v_buf, o_buf, p_buf, o_rows, send1, recv1, send2, recv2, send3, recv3, keep_own, keep_other,
                 ring_sem, down_sem, kv_sem, w_sem, x_ssem, x_rsem, g_ssem, g_rsem, a_sem, s1_sem, r1_sem, s2_sem, r2_sem, s3_sem, r3_sem, in_sem, out_sem):
    tp = lax.axis_index('tp')
    ep = lax.axis_index('ep')
    core = ep % 2
    chip = ep // 2
    mate = chip * 2 + 1 - core
    across = (1 - chip) * 2 + core
    diagonal = (1 - chip) * 2 + 1 - core
    tokens, d_model = h_ref.shape
    n_heads = wq_ref.shape[1] // HEAD
    n_kv = wk_ref.shape[1] // HEAD
    group = n_heads // n_kv
    ctx_rows = kc_ref.shape[1] // 2
    x_ref = x_all.at[ep]
    n_local, _, hidden_dim = wg_ref.shape
    n_tiles = d_model // TILE

    def expert_copies(j, slot):
        return (pltpu.make_async_copy(wg_ref.at[j], ring.at[slot, 0], ring_sem.at[slot, 0]),
                pltpu.make_async_copy(wu_ref.at[j], ring.at[slot, 1], ring_sem.at[slot, 1]))

    def shared_copies(slot):
        return (pltpu.make_async_copy(wsg_ref, ring.at[slot, 0], ring_sem.at[slot, 0]),
                pltpu.make_async_copy(wsu_ref, ring.at[slot, 1], ring_sem.at[slot, 1]))

    def down_copies(i, slot):
        cols = pl.ds(pl.multiple_of(i * TILE, TILE), TILE)
        base = slot * (n_local + 1)
        return (pltpu.make_async_copy(wd_ref.at[:, :, cols], down.at[pl.ds(base, n_local)], down_sem.at[slot, 0]),
                pltpu.make_async_copy(wsd_ref.at[:, cols], down.at[base + n_local], down_sem.at[slot, 1]))

    def cache_copies(g):
        slot = g % KV_SLOTS
        copies = []
        for k in range(KV_PAIRS):
            dst = down.at[slot * KV_PAIRS + k, pl.ds(0, 2 * ctx_rows)]
            for n, ref in enumerate((kc_ref, vc_ref)):
                copies.append(pltpu.make_async_copy(ref.at[g * KV_PAIRS + k], dst.at[:, pl.ds(n * HEAD, HEAD)], kv_sem.at[slot, k, n]))
        return copies

    def start(copies):
        for c in copies:
            c.start()

    def wait(copies):
        for c in copies:
            c.wait()

    qw, kvw = n_heads * HEAD, n_kv * HEAD
    proj = (pltpu.make_async_copy(wq_ref, ring.at[0, 0, :, pl.ds(0, qw)], w_sem.at[0]),
            pltpu.make_async_copy(wk_ref, ring.at[0, 1, :, pl.ds(0, kvw)], w_sem.at[1]),
            pltpu.make_async_copy(wv_ref, ring.at[0, 1, :, pl.ds(kvw, kvw)], w_sem.at[2]))
    out_proj = pltpu.make_async_copy(wo_ref, x_rows, w_sem.at[3])
    small = [pltpu.make_async_copy(src, dst, in_sem.at[k]) for k, (src, dst) in enumerate(
        ((h_in, h_ref), (gain_a_in, gain_a_ref), (ids_in, ids_ref), (gv_in, gv_ref), (len_in, len_ref), (gain_f_in, gain_f_ref)))]
    start(small)
    start(proj)
    for g in range(KV_SLOTS):
        start(cache_copies(g))
    out_proj.start()

    barrier = pltpu.get_barrier_semaphore()
    for dev in ({'ep': mate}, {'ep': across}, {'ep': diagonal}, {'tp': 1 - tp}):
        pl.semaphore_signal(barrier, inc=1, device_id=dev, device_id_type=MESH_ID)

    wait(small)
    block_rows = 16
    expert_row = lax.broadcasted_iota(jnp.int32, gt_ref.shape, 0)
    table = jnp.zeros(gt_ref.shape, jnp.float32)
    for j in range(ids_ref.shape[0]):
        table = table + jnp.where(ids_ref[j:j + 1, :] == expert_row, gv_ref[j:j + 1, :], 0.0)
    gt_ref[...] = table

    def attn_norm(r, carry):
        rows = pl.ds(pl.multiple_of(r * block_rows, block_rows), block_rows)
        x_ref[rows, :] = rms_norm(h_ref[rows, :].astype(jnp.float32), gain_a_ref[...]).astype(jnp.bfloat16)
        return carry
    lax.fori_loop(0, tokens // block_rows, attn_norm, 0)

    pl.semaphore_wait(barrier, 4)

    def remote(src, dst, ssem, rsem, dev):
        return pltpu.make_async_remote_copy(src_ref=src, dst_ref=dst, send_sem=ssem, recv_sem=rsem, device_id=dev, device_id_type=MESH_ID)

    def gate_rows(shard):
        return gt_ref.at[pl.ds(pl.multiple_of((shard * 2 + tp) * n_local, n_local), n_local)]

    g_sends = [remote(gate_rows(peer), gates.at[ep], g_ssem.at[k], g_rsem.at[ep], {'ep': peer}) for k, peer in enumerate((mate, across, diagonal))]
    x_sends = [remote(x_ref, x_all.at[ep], x_ssem.at[k], x_rsem.at[ep], {'ep': peer}) for k, peer in enumerate((mate, across))]
    a_send = remote(attn_ref, attn_rx, a_sem.at[0], a_sem.at[1], {'tp': 1 - tp})
    start(g_sends)
    start(x_sends)

    def recv_wait(dst, sem):
        pltpu.make_async_copy(dst, dst, sem).wait()

    lane = lax.broadcasted_iota(jnp.int32, (tokens, tokens), 1)
    row = lax.broadcasted_iota(jnp.int32, (tokens, tokens), 0)
    before = (row < lane).astype(jnp.bfloat16)
    slot_row = lax.broadcasted_iota(jnp.int32, (SLOT, tokens), 0).astype(jnp.float32)

    def dispatch(s, block):
        rows = pl.ds(pl.multiple_of(s * SLOT, SLOT), SLOT)
        gate = gates[s]
        chosen = (gate > 0.0).astype(jnp.float32)
        pos = jnp.dot(chosen.astype(jnp.bfloat16), before, preferred_element_type=jnp.float32)
        for j in range(n_local):
            hit = (pos[j:j + 1, :] == slot_row) & (chosen[j:j + 1, :] > 0.0)
            place[j * SLOT:(j + 1) * SLOT, :] = jnp.where(hit, 1.0, 0.0)
            picked = jnp.sum(jnp.where(hit, gate[j:j + 1, :], 0.0), axis=-1, keepdims=True)
            slot_gate[j, rows, :] = jnp.broadcast_to(picked, (SLOT, tokens))
        placed = place[...]
        place_t[s] = placed.T.astype(jnp.bfloat16)
        placed = placed.astype(jnp.bfloat16)

        for n in range(n_tiles):
            cols = slice(n * TILE, (n + 1) * TILE)
            got = jnp.dot(placed, block[:, cols], preferred_element_type=jnp.float32).astype(jnp.bfloat16)
            x_rows[:, rows, cols] = got.reshape(n_local, SLOT, TILE)

    x_own = x_ref[...]
    wait(proj)
    for n in range(qw // TILE):
        got = jnp.dot(x_own, ring[0, 0, :, n * TILE:(n + 1) * TILE], preferred_element_type=jnp.float32).astype(jnp.bfloat16).astype(jnp.float32)
        for k in range(TILE // HEAD):
            q_buf[:, n * (TILE // HEAD) + k, :] = got[:, k * HEAD:(k + 1) * HEAD]
    for n, buf in enumerate((k_buf, v_buf)):
        got = jnp.dot(x_own, ring[0, 1, :, n * kvw:(n + 1) * kvw], preferred_element_type=jnp.float32).astype(jnp.bfloat16).astype(jnp.float32)
        for k in range(n_heads):
            buf[:, k, :] = got[:, (k // group) * HEAD:(k // group + 1) * HEAD]

    scale = HEAD ** -0.5
    cache_lane = lax.broadcasted_iota(jnp.int32, (n_heads, ctx_rows), 1)
    head_row = lax.broadcasted_iota(jnp.int32, (n_heads, ctx_rows), 0)
    cache_pos = jnp.where(cache_lane % n_kv == head_row // group, cache_lane // n_kv, ctx_rows)

    def attend(i, carry):
        for g in range(2):
            wait(cache_copies(2 * i + g))
        first = i * BATCH
        base = (2 * i % KV_SLOTS) * KV_PAIRS

        def cache(u, n):
            return down[base + u // 2, (u % 2) * ctx_rows:(u % 2 + 1) * ctx_rows, n * HEAD:(n + 1) * HEAD]

        q_all = q_buf[pl.ds(pl.multiple_of(first, BATCH), BATCH)].reshape(BATCH * n_heads, HEAD).astype(jnp.bfloat16)
        stats = []
        for u in range(BATCH):
            t = first + u
            own_rows = slice(u * n_heads, (u + 1) * n_heads)
            s = lax.dot_general(q_all, cache(u, 0), (((1,), (1,)), ((), ())), preferred_element_type=jnp.float32)[own_rows] * scale
            s = jnp.where(cache_pos < len_ref[t], s, -jnp.inf)
            own = jnp.sum(q_buf[t] * k_buf[t], axis=-1, keepdims=True) * scale
            top = jnp.maximum(jnp.max(s, axis=-1, keepdims=True), own)
            w = jnp.exp(s - top)
            w_own = jnp.exp(own - top)
            p_buf[own_rows, :] = w
            stats.append((w_own, jnp.sum(w, axis=-1, keepdims=True) + w_own))
        p_all = p_buf[...].astype(jnp.bfloat16)
        for u in range(0, BATCH, 2):
            pair = jnp.concatenate([cache(u, 1), cache(u + 1, 1)], axis=1)
            mixed = jnp.dot(p_all, pair, preferred_element_type=jnp.float32)
            for e in range(2):
                w_own, norm = stats[u + e]
                mine = mixed[(u + e) * n_heads:(u + e + 1) * n_heads, e * HEAD:(e + 1) * HEAD]
                t = first + u + e
                o_buf[t] = (mine + w_own.astype(jnp.bfloat16).astype(jnp.float32) * v_buf[t]) / norm

        @pl.when(2 * i + KV_SLOTS < n_groups)
        def _():
            for g in range(2):
                start(cache_copies(2 * i + KV_SLOTS + g))

        @pl.when(i == n_groups // 2 - 4)
        def _():
            start(expert_copies(0, 0))

        @pl.when(i == n_groups // 2 - 3)
        def _():
            start(expert_copies(1, 1))
        return carry
    n_groups = tokens // (2 * KV_PAIRS)
    lax.fori_loop(0, n_groups // 2, attend, 0)

    recv_wait(x_all.at[across], x_rsem.at[across])
    x_fwd = remote(x_all.at[across], x_all.at[across], x_ssem.at[2], x_rsem.at[across], {'ep': mate})
    x_fwd.start()

    for k in range(n_heads):
        o_rows[:, k * HEAD:(k + 1) * HEAD] = o_buf[:, k, :].astype(jnp.bfloat16)
    out_proj.wait()
    for n in range(n_tiles):
        cols = slice(n * TILE, (n + 1) * TILE)
        got = jnp.dot(o_rows[...], x_rows[:, :, cols].reshape(qw, TILE), preferred_element_type=jnp.float32)
        attn_ref[:, cols] = got.astype(jnp.bfloat16)

    gates[ep] = gt_ref[pl.ds(pl.multiple_of((ep * 2 + tp) * n_local, n_local), n_local), :]
    dispatch(ep, x_ref)
    for src in (mate, across, diagonal):
        recv_wait(gates.at[src], g_rsem.at[src])
    recv_wait(x_all.at[mate], x_rsem.at[mate])
    dispatch(mate, x_all.at[mate])
    a_send.start()
    dispatch(across, x_all.at[across])
    recv_wait(x_all.at[diagonal], x_rsem.at[diagonal])
    dispatch(diagonal, x_all.at[diagonal])

    def gate_up(lhs, slot, dst):
        full = hidden_dim // TILE * TILE
        for c in range(0, full, TILE):
            cols = slice(c, c + TILE)
            g = jnp.dot(lhs[...], ring[slot, 0, :, cols], preferred_element_type=jnp.float32)
            u = jnp.dot(lhs[...], ring[slot, 1, :, cols], preferred_element_type=jnp.float32)
            act[dst, :, cols] = (jax.nn.silu(g) * u).astype(jnp.bfloat16)
        if full < hidden_dim:
            cols = slice(full, hidden_dim)
            both = jnp.concatenate([ring[slot, 0, :, cols], ring[slot, 1, :, cols]], axis=1)
            gu = jnp.dot(lhs[...], both, preferred_element_type=jnp.float32)
            rest = hidden_dim - full
            act[dst, :, cols] = (jax.nn.silu(gu[:, :rest]) * gu[:, rest:]).astype(jnp.bfloat16)

    def expert(j, carry):
        slot = j % 2
        wait(expert_copies(j, slot))
        gate_up(x_rows.at[j], slot, j)

        @pl.when(j + 2 < n_local)
        def _():
            start(expert_copies(j + 2, slot))

        @pl.when(j + 2 == n_local)
        def _():
            start(shared_copies(slot))
        return carry
    lax.fori_loop(0, n_local, expert, 0)
    shared_slot = n_local % 2
    start(down_copies(0, 0))

    recv_wait(attn_rx, a_sem.at[1])

    def ffn_norm(r, carry):
        rows = pl.ds(pl.multiple_of(r * block_rows, block_rows), block_rows)
        attn = (attn_ref[rows, :].astype(jnp.float32) + attn_rx[rows, :].astype(jnp.float32)).astype(jnp.bfloat16).astype(jnp.float32)
        res = h_ref[rows, :].astype(jnp.float32) + attn
        attn_sum[rows, :] = res
        y_norm[rows, :] = rms_norm(res, gain_f_ref[...]).astype(jnp.bfloat16)
        return carry
    lax.fori_loop(0, tokens // block_rows, ffn_norm, 0)
    wait(shared_copies(shared_slot))
    gate_up(y_norm, shared_slot, n_local)
    start(down_copies(1, 1))

    def split3(v):
        a = v.astype(jnp.bfloat16)
        r = v - a.astype(jnp.float32)
        b = r.astype(jnp.bfloat16)
        c = (r - b.astype(jnp.float32)).astype(jnp.bfloat16)
        return a, b, c

    def combine(s):
        rows = pl.ds(pl.multiple_of(s * SLOT, SLOT), SLOT)
        sums = [jnp.dot(place_t[s], y_parts[p, :, rows, :].reshape(n_local * SLOT, TILE), preferred_element_type=jnp.float32) for p in range(3)]
        return sums[0] + (sums[1] + sums[2])

    def s1_copy(i):
        return remote(send1.at[i], recv1.at[i], s1_sem.at[i], r1_sem.at[i], {'ep': mate})

    def s2_copy(i):
        return remote(send2.at[i], recv2.at[i], s2_sem.at[i], r2_sem.at[i], {'ep': across})

    def s3_copy(i):
        return remote(send3.at[i], recv3.at[i], s3_sem.at[i], r3_sem.at[i], {'tp': 1 - tp})

    def out_copy(i):
        cols = pl.ds(pl.multiple_of(i * TILE, TILE), TILE)
        return pltpu.make_async_copy(out_buf.at[:, cols], out_ref.at[:, cols], out_sem.at[i])

    def down_tile(i, slot):
        wait(down_copies(i, slot))

        for j in range(n_local):
            out = jnp.dot(act[j], down[slot * (n_local + 1) + j], preferred_element_type=jnp.float32)
            gate = slot_gate[j]
            parts = split3(out * jnp.concatenate([gate] * (TILE // tokens), axis=-1))
            for p in range(3):
                y_parts[p, j] = parts[p]
        for b in range(2):
            send1[i, b] = combine(b * 2 + 1 - core).astype(jnp.bfloat16)
        s1_copy(i).start()
        keep_other[i] = combine((1 - chip) * 2 + core)
        keep_own[i] = combine(ep) + jnp.dot(act[n_local], down[slot * (n_local + 1) + n_local], preferred_element_type=jnp.float32)

        @pl.when(i + 2 < n_tiles)
        def _():
            start(down_copies(i + 2, slot))

    def step(i, carry):
        @pl.when(i < n_tiles)
        def _():
            down_tile(i, i % 2)

        @pl.when((i >= LAG1) & (i < n_tiles + LAG1))
        def _():
            k = i - LAG1
            recv_wait(recv1.at[k], r1_sem.at[k])
            send2[k] = (keep_other[k] + recv1[k, 1 - chip].astype(jnp.float32)).astype(jnp.bfloat16)
            s2_copy(k).start()
            keep_own[k] = keep_own[k] + recv1[k, chip].astype(jnp.float32)

        @pl.when((i >= LAG2) & (i < n_tiles + LAG2))
        def _():
            k = i - LAG2
            recv_wait(recv2.at[k], r2_sem.at[k])
            send3[k] = (keep_own[k] + recv2[k].astype(jnp.float32)).astype(jnp.bfloat16)
            s3_copy(k).start()

        @pl.when(i >= LAG3)
        def _():
            k = i - LAG3
            cols = pl.ds(pl.multiple_of(k * TILE, TILE), TILE)
            recv_wait(recv3.at[k], r3_sem.at[k])
            ffn = send3[k].astype(jnp.float32) + recv3[k].astype(jnp.float32)
            out_buf[:, cols] = (attn_sum[:, cols] + ffn).astype(jnp.bfloat16)
            out_copy(k).start()
        return carry
    lax.fori_loop(0, n_tiles + LAG3, step, 0)

    for c in g_sends + x_sends + [x_fwd, a_send]:
        c.wait_send()

    def drain(i, carry):
        s1_copy(i).wait_send()
        s2_copy(i).wait_send()
        s3_copy(i).wait_send()
        out_copy(i).wait()
        return carry
    lax.fori_loop(0, n_tiles, drain, 0)


def fused_layer(hidden, g_attn, w_q, w_k, w_v, w_o, k_cache, v_cache, lengths, g_ffn, ws_gate, ws_up, ws_down, w_gate, w_up, w_down, expert_ids, gate_vals, shards):
    tokens, d_model = hidden.shape
    n_local, _, hidden_dim = w_gate.shape
    n_tiles = d_model // TILE
    n_heads = w_q.shape[1] // HEAD
    ctx_len, n_kv = k_cache.shape[1:3]
    bf16, f32 = jnp.bfloat16, jnp.float32
    dma = pltpu.SemaphoreType.DMA
    hbm = pl.BlockSpec(memory_space=pltpu.HBM)
    tile = pltpu.VMEM((n_tiles, tokens, TILE), bf16)
    tile_f32 = pltpu.VMEM((n_tiles, tokens, TILE), f32)
    pair_tile = pltpu.VMEM((n_tiles, 2, tokens, TILE), bf16)
    rows_bf16 = pltpu.VMEM((tokens, d_model), bf16)
    heads = pltpu.VMEM((tokens, n_heads, HEAD), f32)
    caches = [c.reshape(tokens // 2, 2 * ctx_len * n_kv, HEAD) for c in (k_cache, v_cache)]
    return pl.pallas_call(
        layer_kernel,
        out_shape=jax.ShapeDtypeStruct((tokens, d_model), bf16),
        in_specs=[hbm] * 18,
        out_specs=hbm,
        scratch_shapes=[
            pltpu.VMEM((4, tokens, d_model), bf16),
            pltpu.VMEM((n_local, 4 * SLOT, d_model), bf16),
            pltpu.VMEM((n_local + 1, tokens, hidden_dim), bf16),
            pltpu.VMEM((4, tokens, n_local * SLOT), bf16),
            pltpu.VMEM((n_local, 4 * SLOT, tokens), f32),
            pltpu.VMEM((n_local * SLOT, tokens), f32),
            pltpu.VMEM((3, n_local, 4 * SLOT, TILE), bf16),
            pltpu.VMEM((2, 2, d_model, hidden_dim), bf16),
            pltpu.VMEM((2 * (n_local + 1), hidden_dim, TILE), bf16),
            rows_bf16, rows_bf16,
            pltpu.VMEM((tokens, d_model), f32),
            rows_bf16,
            pltpu.VMEM((4, n_local, tokens), f32),
            pltpu.VMEM((n_local * shards, tokens), f32),
            pltpu.SMEM((tokens,), jnp.int32), rows_bf16, pltpu.VMEM((1, d_model), f32), pltpu.VMEM((1, d_model), f32),
            pltpu.VMEM(expert_ids.shape[::-1], jnp.int32), pltpu.VMEM(gate_vals.shape[::-1], f32), rows_bf16,
            heads, heads, heads, heads,
            pltpu.VMEM((BATCH * n_heads, ctx_len * n_kv), f32),
            pltpu.VMEM((tokens, n_heads * HEAD), bf16),
            pair_tile, pair_tile, tile, tile, tile, tile, tile_f32, tile_f32,
            dma((2, 2)), dma((2, 2)), dma((KV_SLOTS, KV_PAIRS, 2)), dma((4,)), dma((3,)), dma((4,)), dma((3,)), dma((4,)), dma((2,)),
        ] + [dma((n_tiles,))] * 6 + [dma((6,)), dma((n_tiles,))],
        compiler_params=pltpu.CompilerParams(collective_id=0, has_side_effects=True, vmem_limit_bytes=63 * 1024 * 1024),
        cost_estimate=pl.CostEstimate(flops=2 * tokens * (n_local + 1) * 3 * d_model * hidden_dim, bytes_accessed=(n_local + 1) * 6 * d_model * hidden_dim, transcendentals=0),
        name='layer',
    )(lengths, hidden, g_attn.reshape(1, d_model), g_ffn.reshape(1, d_model), expert_ids.T, gate_vals.T, w_q, w_k, w_v, w_o.reshape(n_heads, HEAD, d_model), *caches, ws_gate, ws_up, ws_down, w_gate, w_up, w_down)


def solution(mesh):
    tok_spec = P(('rep', 'ep'), None)
    cache_spec = P(('rep', 'ep'), None, 'tp', None)
    expert_spec = P(('ep', 'tp'), None, None)
    layer = functools.partial(fused_layer, shards=mesh.shape['ep'] * mesh.shape['tp'])
    in_specs = (tok_spec, P(None), P(None, 'tp'), P(None, 'tp'), P(None, 'tp'), P('tp', None), cache_spec, cache_spec, P(('rep', 'ep')), P(None), P(None, 'tp'), P(None, 'tp'), P('tp', None), expert_spec, expert_spec, expert_spec, tok_spec, tok_spec)
    return jax.shard_map(layer, mesh=mesh, in_specs=in_specs, out_specs=tok_spec, check_vma=False)
```

```python
import functools

import jax
import jax.numpy as jnp
from jax import lax
from jax.experimental import pallas as pl
from jax.experimental.pallas import tpu as pltpu
from jax.sharding import PartitionSpec as P

EPS = 1e-6
TILE = 256
SLOT = 32
HEAD = 128
BATCH = 16
GROUP = 3
LAG1, LAG2, LAG3 = 1, 4, 7
MESH_ID = pl.DeviceIdType.MESH


def rms_norm(values, gain):
    return values * lax.rsqrt(jnp.mean(values * values, axis=-1, keepdims=True) + EPS) * gain


def layer_kernel(len_in, h_in, gain_a_in, gain_f_in, ids_in, gv_in, wq_ref, wk_ref, wv_ref, wo_ref, kc_ref, vc_ref,
                 wsg_ref, wsu_ref, wsd_ref, wg_ref, wu_ref, wd_ref, out_ref,
                 x_all, x_rows, act, place_t, slot_gate, place, y_parts, ring, down, attn_ref, attn_rx, attn_sum, y_norm, gates, gt_ref,
                 len_ref, h_ref, gain_a_ref, gain_f_ref, ids_ref, gv_ref, out_buf, q_buf, k_buf, v_buf, o_buf, p_buf, o_rows, send1, recv1, send2, recv2, send3, recv3, keep_own, keep_other,
                 ring_sem, down_sem, kv_sem, w_sem, x_ssem, x_rsem, g_ssem, g_rsem, a_sem, s1_sem, r1_sem, s2_sem, r2_sem, s3_sem, r3_sem, in_sem, out_sem):
    tp = lax.axis_index('tp')
    ep = lax.axis_index('ep')
    core = ep % 2
    chip = ep // 2
    mate = chip * 2 + 1 - core
    across = (1 - chip) * 2 + core
    diagonal = (1 - chip) * 2 + 1 - core
    tokens, d_model = h_ref.shape
    n_heads = wq_ref.shape[1] // HEAD
    n_kv = wk_ref.shape[1] // HEAD
    group = n_heads // n_kv
    ctx_rows = kc_ref.shape[1] // 2
    x_ref = x_all.at[ep]
    n_local, _, hidden_dim = wg_ref.shape
    n_tiles = d_model // TILE

    def expert_copies(j, slot):
        return (pltpu.make_async_copy(wg_ref.at[j], ring.at[slot, 0], ring_sem.at[slot, 0]),
                pltpu.make_async_copy(wu_ref.at[j], ring.at[slot, 1], ring_sem.at[slot, 1]))

    def shared_copies(slot):
        return (pltpu.make_async_copy(wsg_ref, ring.at[slot, 0], ring_sem.at[slot, 0]),
                pltpu.make_async_copy(wsu_ref, ring.at[slot, 1], ring_sem.at[slot, 1]))

    def down_copies(i, slot):
        cols = pl.ds(pl.multiple_of(i * TILE, TILE), TILE)
        base = slot * (n_local + 1)
        parts = [(j, min(GROUP, n_local - j)) for j in range(0, n_local, GROUP)]
        copies = [[pltpu.make_async_copy(wd_ref.at[pl.ds(j, n), :, cols], down.at[pl.ds(base + j, n)], down_sem.at[slot, k])] for k, (j, n) in enumerate(parts)]
        copies[-1].append(pltpu.make_async_copy(wsd_ref.at[:, cols], down.at[base + n_local], down_sem.at[slot, len(parts)]))
        return copies

    def down_start(i, slot):
        for part in down_copies(i, slot):
            start(part)

    def cache_copies(i, n):
        slot = i % 2
        pairs = BATCH // 2
        copies = []
        for k in range(pairs):
            dst = down.at[slot * pairs + k, pl.ds(0, 2 * ctx_rows)]
            copies.append(pltpu.make_async_copy((kc_ref, vc_ref)[n].at[i * pairs + k], dst.at[:, pl.ds(n * HEAD, HEAD)], kv_sem.at[slot, k, n]))
        return copies

    def start(copies):
        for c in copies:
            c.start()

    def wait(copies):
        for c in copies:
            c.wait()

    qw, kvw = n_heads * HEAD, n_kv * HEAD
    proj = (pltpu.make_async_copy(wq_ref, ring.at[0, 0, :, pl.ds(0, qw)], w_sem.at[0]),
            pltpu.make_async_copy(wk_ref, ring.at[0, 1, :, pl.ds(0, kvw)], w_sem.at[1]),
            pltpu.make_async_copy(wv_ref, ring.at[0, 1, :, pl.ds(kvw, kvw)], w_sem.at[2]))
    out_proj = pltpu.make_async_copy(wo_ref, x_rows, w_sem.at[3])
    small = [pltpu.make_async_copy(src, dst, in_sem.at[k]) for k, (src, dst) in enumerate(
        ((h_in, h_ref), (gain_a_in, gain_a_ref), (ids_in, ids_ref), (gv_in, gv_ref), (len_in, len_ref), (gain_f_in, gain_f_ref)))]
    start(small)
    start(proj)
    for i in range(2):
        start(cache_copies(i, 0))
        start(cache_copies(i, 1))
    out_proj.start()

    barrier = pltpu.get_barrier_semaphore()
    for dev in ({'ep': mate}, {'ep': across}, {'ep': diagonal}, {'tp': 1 - tp}):
        pl.semaphore_signal(barrier, inc=1, device_id=dev, device_id_type=MESH_ID)

    wait(small)
    block_rows = 16
    expert_row = lax.broadcasted_iota(jnp.int32, gt_ref.shape, 0)
    table = jnp.zeros(gt_ref.shape, jnp.float32)
    for j in range(ids_ref.shape[0]):
        table = table + jnp.where(ids_ref[j:j + 1, :] == expert_row, gv_ref[j:j + 1, :], 0.0)
    gt_ref[...] = table

    def attn_norm(r, carry):
        rows = pl.ds(pl.multiple_of(r * block_rows, block_rows), block_rows)
        x_ref[rows, :] = rms_norm(h_ref[rows, :].astype(jnp.float32), gain_a_ref[...]).astype(jnp.bfloat16)
        return carry
    lax.fori_loop(0, tokens // block_rows, attn_norm, 0)

    pl.semaphore_wait(barrier, 4)

    def remote(src, dst, ssem, rsem, dev):
        return pltpu.make_async_remote_copy(src_ref=src, dst_ref=dst, send_sem=ssem, recv_sem=rsem, device_id=dev, device_id_type=MESH_ID)

    def gate_rows(shard):
        return gt_ref.at[pl.ds(pl.multiple_of((shard * 2 + tp) * n_local, n_local), n_local)]

    g_sends = [remote(gate_rows(peer), gates.at[ep], g_ssem.at[k], g_rsem.at[ep], {'ep': peer}) for k, peer in enumerate((mate, across, diagonal))]
    x_sends = [remote(x_ref, x_all.at[ep], x_ssem.at[k], x_rsem.at[ep], {'ep': peer}) for k, peer in enumerate((mate, across))]
    a_send = remote(attn_ref, attn_rx, a_sem.at[0], a_sem.at[1], {'tp': 1 - tp})
    start(g_sends)
    start(x_sends)

    def recv_wait(dst, sem):
        pltpu.make_async_copy(dst, dst, sem).wait()

    lane = lax.broadcasted_iota(jnp.int32, (tokens, tokens), 1)
    row = lax.broadcasted_iota(jnp.int32, (tokens, tokens), 0)
    before = (row < lane).astype(jnp.bfloat16)
    slot_row = lax.broadcasted_iota(jnp.int32, (SLOT, tokens), 0).astype(jnp.float32)

    def dispatch(s, block):
        rows = pl.ds(pl.multiple_of(s * SLOT, SLOT), SLOT)
        gate = gates[s]
        chosen = (gate > 0.0).astype(jnp.float32)
        pos = jnp.dot(chosen.astype(jnp.bfloat16), before, preferred_element_type=jnp.float32)
        for j in range(n_local):
            hit = (pos[j:j + 1, :] == slot_row) & (chosen[j:j + 1, :] > 0.0)
            place[j * SLOT:(j + 1) * SLOT, :] = jnp.where(hit, 1.0, 0.0)
            picked = jnp.sum(jnp.where(hit, gate[j:j + 1, :], 0.0), axis=-1, keepdims=True)
            slot_gate[j, rows, :] = jnp.broadcast_to(picked, (SLOT, tokens))
        placed = place[...]
        place_t[s] = placed.T.astype(jnp.bfloat16)
        placed = placed.astype(jnp.bfloat16)

        for n in range(n_tiles):
            cols = slice(n * TILE, (n + 1) * TILE)
            got = jnp.dot(placed, block[:, cols], preferred_element_type=jnp.float32).astype(jnp.bfloat16)
            x_rows[:, rows, cols] = got.reshape(n_local, SLOT, TILE)

    x_own = x_ref[...]
    wait(proj)
    for n in range(qw // TILE):
        got = jnp.dot(x_own, ring[0, 0, :, n * TILE:(n + 1) * TILE], preferred_element_type=jnp.float32).astype(jnp.bfloat16).astype(jnp.float32)
        for k in range(TILE // HEAD):
            q_buf[:, n * (TILE // HEAD) + k, :] = got[:, k * HEAD:(k + 1) * HEAD]
    for n, buf in enumerate((k_buf, v_buf)):
        got = jnp.dot(x_own, ring[0, 1, :, n * kvw:(n + 1) * kvw], preferred_element_type=jnp.float32).astype(jnp.bfloat16).astype(jnp.float32)
        for k in range(n_heads):
            buf[:, k, :] = got[:, (k // group) * HEAD:(k // group + 1) * HEAD]

    scale = HEAD ** -0.5
    cache_lane = lax.broadcasted_iota(jnp.int32, (n_heads, ctx_rows), 1)
    head_row = lax.broadcasted_iota(jnp.int32, (n_heads, ctx_rows), 0)
    cache_pos = jnp.where(cache_lane % n_kv == head_row // group, cache_lane // n_kv, ctx_rows)

    def attend(i, carry):
        first = i * BATCH
        base = (i % 2) * (BATCH // 2)
        wait(cache_copies(i, 0))

        def cache(u, n):
            return down[base + u // 2, (u % 2) * ctx_rows:(u % 2 + 1) * ctx_rows, n * HEAD:(n + 1) * HEAD]

        q_all = q_buf[pl.ds(pl.multiple_of(first, BATCH), BATCH)].reshape(BATCH * n_heads, HEAD).astype(jnp.bfloat16)
        stats = []
        for u in range(BATCH):
            t = first + u
            own_rows = slice(u * n_heads, (u + 1) * n_heads)
            s = lax.dot_general(q_all, cache(u, 0), (((1,), (1,)), ((), ())), preferred_element_type=jnp.float32)[own_rows] * scale
            s = jnp.where(cache_pos < len_ref[t], s, -jnp.inf)
            own = jnp.sum(q_buf[t] * k_buf[t], axis=-1, keepdims=True) * scale
            top = jnp.maximum(jnp.max(s, axis=-1, keepdims=True), own)
            w = jnp.exp(s - top)
            w_own = jnp.exp(own - top)
            p_buf[own_rows, :] = w
            stats.append((w_own, jnp.sum(w, axis=-1, keepdims=True) + w_own))

        @pl.when(i + 2 < n_batches)
        def _():
            start(cache_copies(i + 2, 0))

        wait(cache_copies(i, 1))
        p_all = p_buf[...].astype(jnp.bfloat16)
        for u in range(0, BATCH, 2):
            pair = jnp.concatenate([cache(u, 1), cache(u + 1, 1)], axis=1)
            mixed = jnp.dot(p_all, pair, preferred_element_type=jnp.float32)
            for e in range(2):
                w_own, norm = stats[u + e]
                mine = mixed[(u + e) * n_heads:(u + e + 1) * n_heads, e * HEAD:(e + 1) * HEAD]
                t = first + u + e
                o_buf[t] = (mine + w_own.astype(jnp.bfloat16).astype(jnp.float32) * v_buf[t]) / norm

        @pl.when(i + 2 < n_batches)
        def _():
            start(cache_copies(i + 2, 1))

        @pl.when(i == n_batches - 3)
        def _():
            start(expert_copies(0, 0))
            start(expert_copies(1, 1))
        return carry
    n_batches = tokens // BATCH
    lax.fori_loop(0, n_batches, attend, 0)

    for k in range(n_heads):
        o_rows[:, k * HEAD:(k + 1) * HEAD] = o_buf[:, k, :].astype(jnp.bfloat16)
    out_proj.wait()
    for n in range(n_tiles):
        cols = slice(n * TILE, (n + 1) * TILE)
        got = jnp.dot(o_rows[...], x_rows[:, :, cols].reshape(qw, TILE), preferred_element_type=jnp.float32)
        attn_ref[:, cols] = got.astype(jnp.bfloat16)

    recv_wait(x_all.at[across], x_rsem.at[across])
    x_fwd = remote(x_all.at[across], x_all.at[across], x_ssem.at[2], x_rsem.at[across], {'ep': mate})
    x_fwd.start()

    gates[ep] = gt_ref[pl.ds(pl.multiple_of((ep * 2 + tp) * n_local, n_local), n_local), :]
    dispatch(ep, x_ref)
    for src in (mate, across, diagonal):
        recv_wait(gates.at[src], g_rsem.at[src])
    recv_wait(x_all.at[mate], x_rsem.at[mate])
    dispatch(mate, x_all.at[mate])
    a_send.start()
    dispatch(across, x_all.at[across])
    recv_wait(x_all.at[diagonal], x_rsem.at[diagonal])
    dispatch(diagonal, x_all.at[diagonal])

    def gate_up(lhs, slot, dst):
        full = hidden_dim // TILE * TILE
        for c in range(0, full, TILE):
            cols = slice(c, c + TILE)
            g = jnp.dot(lhs[...], ring[slot, 0, :, cols], preferred_element_type=jnp.float32)
            u = jnp.dot(lhs[...], ring[slot, 1, :, cols], preferred_element_type=jnp.float32)
            act[dst, :, cols] = (jax.nn.silu(g) * u).astype(jnp.bfloat16)
        if full < hidden_dim:
            cols = slice(full, hidden_dim)
            both = jnp.concatenate([ring[slot, 0, :, cols], ring[slot, 1, :, cols]], axis=1)
            gu = jnp.dot(lhs[...], both, preferred_element_type=jnp.float32)
            rest = hidden_dim - full
            act[dst, :, cols] = (jax.nn.silu(gu[:, :rest]) * gu[:, rest:]).astype(jnp.bfloat16)

    def expert(j, carry):
        slot = j % 2
        wait(expert_copies(j, slot))
        gate_up(x_rows.at[j], slot, j)

        @pl.when(j + 2 < n_local)
        def _():
            start(expert_copies(j + 2, slot))

        @pl.when(j + 2 == n_local)
        def _():
            start(shared_copies(slot))
        return carry
    lax.fori_loop(0, n_local, expert, 0)
    shared_slot = n_local % 2
    down_start(0, 0)

    recv_wait(attn_rx, a_sem.at[1])

    def ffn_norm(r, carry):
        rows = pl.ds(pl.multiple_of(r * block_rows, block_rows), block_rows)
        attn = (attn_ref[rows, :].astype(jnp.float32) + attn_rx[rows, :].astype(jnp.float32)).astype(jnp.bfloat16).astype(jnp.float32)
        res = h_ref[rows, :].astype(jnp.float32) + attn
        attn_sum[rows, :] = res
        y_norm[rows, :] = rms_norm(res, gain_f_ref[...]).astype(jnp.bfloat16)
        return carry
    lax.fori_loop(0, tokens // block_rows, ffn_norm, 0)
    wait(shared_copies(shared_slot))
    gate_up(y_norm, shared_slot, n_local)
    down_start(1, 1)

    def split3(v):
        a = v.astype(jnp.bfloat16)
        r = v - a.astype(jnp.float32)
        b = r.astype(jnp.bfloat16)
        c = (r - b.astype(jnp.float32)).astype(jnp.bfloat16)
        return a, b, c

    def combine(s):
        rows = pl.ds(pl.multiple_of(s * SLOT, SLOT), SLOT)
        sums = [jnp.dot(place_t[s], y_parts[p, :, rows, :].reshape(n_local * SLOT, TILE), preferred_element_type=jnp.float32) for p in range(3)]
        return sums[0] + (sums[1] + sums[2])

    def s1_copy(i):
        return remote(send1.at[i], recv1.at[i], s1_sem.at[i], r1_sem.at[i], {'ep': mate})

    def s2_copy(i):
        return remote(send2.at[i], recv2.at[i], s2_sem.at[i], r2_sem.at[i], {'ep': across})

    def s3_copy(i):
        return remote(send3.at[i], recv3.at[i], s3_sem.at[i], r3_sem.at[i], {'tp': 1 - tp})

    def out_copy(i):
        cols = pl.ds(pl.multiple_of(i * TILE, TILE), TILE)
        return pltpu.make_async_copy(out_buf.at[:, cols], out_ref.at[:, cols], out_sem.at[i])

    def down_tile(i, slot):
        base = slot * (n_local + 1)
        now, later = down_copies(i, slot), down_copies(i + 2, slot)
        for k in range(len(now)):
            wait(now[k])
            for j in range(k * GROUP, min((k + 1) * GROUP, n_local)):
                out = jnp.dot(act[j], down[base + j], preferred_element_type=jnp.float32)
                parts = split3(out * jnp.concatenate([slot_gate[j]] * (TILE // tokens), axis=-1))
                for p in range(3):
                    y_parts[p, j] = parts[p]
            if k == len(now) - 1:
                keep_own[i] = jnp.dot(act[n_local], down[base + n_local], preferred_element_type=jnp.float32)

            @pl.when(i + 2 < n_tiles)
            def _(k=k):
                start(later[k])
        for b in range(2):
            send1[i, b] = combine(b * 2 + 1 - core).astype(jnp.bfloat16)
        s1_copy(i).start()
        keep_other[i] = combine((1 - chip) * 2 + core)
        keep_own[i] = keep_own[i] + combine(ep)

    def step(i, carry):
        @pl.when(i < n_tiles)
        def _():
            down_tile(i, i % 2)

        @pl.when((i >= LAG1) & (i < n_tiles + LAG1))
        def _():
            k = i - LAG1
            recv_wait(recv1.at[k], r1_sem.at[k])
            send2[k] = (keep_other[k] + recv1[k, 1 - chip].astype(jnp.float32)).astype(jnp.bfloat16)
            s2_copy(k).start()
            keep_own[k] = keep_own[k] + recv1[k, chip].astype(jnp.float32)

        @pl.when((i >= LAG2) & (i < n_tiles + LAG2))
        def _():
            k = i - LAG2
            recv_wait(recv2.at[k], r2_sem.at[k])
            send3[k] = (keep_own[k] + recv2[k].astype(jnp.float32)).astype(jnp.bfloat16)
            s3_copy(k).start()

        @pl.when(i >= LAG3)
        def _():
            k = i - LAG3
            cols = pl.ds(pl.multiple_of(k * TILE, TILE), TILE)
            recv_wait(recv3.at[k], r3_sem.at[k])
            ffn = send3[k].astype(jnp.float32) + recv3[k].astype(jnp.float32)
            out_buf[:, cols] = (attn_sum[:, cols] + ffn).astype(jnp.bfloat16)
            out_copy(k).start()
        return carry
    lax.fori_loop(0, n_tiles + LAG3, step, 0)

    for c in g_sends + x_sends + [x_fwd, a_send]:
        c.wait_send()

    def drain(i, carry):
        s1_copy(i).wait_send()
        s2_copy(i).wait_send()
        s3_copy(i).wait_send()
        out_copy(i).wait()
        return carry
    lax.fori_loop(0, n_tiles, drain, 0)


def fused_layer(hidden, g_attn, w_q, w_k, w_v, w_o, k_cache, v_cache, lengths, g_ffn, ws_gate, ws_up, ws_down, w_gate, w_up, w_down, expert_ids, gate_vals, shards):
    tokens, d_model = hidden.shape
    n_local, _, hidden_dim = w_gate.shape
    n_tiles = d_model // TILE
    n_heads = w_q.shape[1] // HEAD
    ctx_len, n_kv = k_cache.shape[1:3]
    bf16, f32 = jnp.bfloat16, jnp.float32
    dma = pltpu.SemaphoreType.DMA
    hbm = pl.BlockSpec(memory_space=pltpu.HBM)
    tile = pltpu.VMEM((n_tiles, tokens, TILE), bf16)
    tile_f32 = pltpu.VMEM((n_tiles, tokens, TILE), f32)
    pair_tile = pltpu.VMEM((n_tiles, 2, tokens, TILE), bf16)
    rows_bf16 = pltpu.VMEM((tokens, d_model), bf16)
    heads = pltpu.VMEM((tokens, n_heads, HEAD), f32)
    caches = [c.reshape(tokens // 2, 2 * ctx_len * n_kv, HEAD) for c in (k_cache, v_cache)]
    return pl.pallas_call(
        layer_kernel,
        out_shape=jax.ShapeDtypeStruct((tokens, d_model), bf16),
        in_specs=[hbm] * 18,
        out_specs=hbm,
        scratch_shapes=[
            pltpu.VMEM((4, tokens, d_model), bf16),
            pltpu.VMEM((n_local, 4 * SLOT, d_model), bf16),
            pltpu.VMEM((n_local + 1, tokens, hidden_dim), bf16),
            pltpu.VMEM((4, tokens, n_local * SLOT), bf16),
            pltpu.VMEM((n_local, 4 * SLOT, tokens), f32),
            pltpu.VMEM((n_local * SLOT, tokens), f32),
            pltpu.VMEM((3, n_local, 4 * SLOT, TILE), bf16),
            pltpu.VMEM((2, 2, d_model, hidden_dim), bf16),
            pltpu.VMEM((2 * (n_local + 1), hidden_dim, TILE), bf16),
            rows_bf16, rows_bf16,
            pltpu.VMEM((tokens, d_model), f32),
            rows_bf16,
            pltpu.VMEM((4, n_local, tokens), f32),
            pltpu.VMEM((n_local * shards, tokens), f32),
            pltpu.SMEM((tokens,), jnp.int32), rows_bf16, pltpu.VMEM((1, d_model), f32), pltpu.VMEM((1, d_model), f32),
            pltpu.VMEM(expert_ids.shape[::-1], jnp.int32), pltpu.VMEM(gate_vals.shape[::-1], f32), rows_bf16,
            heads, heads, heads, heads,
            pltpu.VMEM((BATCH * n_heads, ctx_len * n_kv), f32),
            pltpu.VMEM((tokens, n_heads * HEAD), bf16),
            pair_tile, pair_tile, tile, tile, tile, tile, tile_f32, tile_f32,
            dma((2, 2)), dma((2, 4)), dma((2, BATCH // 2, 2)), dma((4,)), dma((3,)), dma((4,)), dma((3,)), dma((4,)), dma((2,)),
        ] + [dma((n_tiles,))] * 6 + [dma((6,)), dma((n_tiles,))],
        compiler_params=pltpu.CompilerParams(collective_id=0, has_side_effects=True, vmem_limit_bytes=63 * 1024 * 1024),
        cost_estimate=pl.CostEstimate(flops=2 * tokens * (n_local + 1) * 3 * d_model * hidden_dim, bytes_accessed=(n_local + 1) * 6 * d_model * hidden_dim, transcendentals=0),
        name='layer',
    )(lengths, hidden, g_attn.reshape(1, d_model), g_ffn.reshape(1, d_model), expert_ids.T, gate_vals.T, w_q, w_k, w_v, w_o.reshape(n_heads, HEAD, d_model), *caches, ws_gate, ws_up, ws_down, w_gate, w_up, w_down)


def solution(mesh):
    tok_spec = P(('rep', 'ep'), None)
    cache_spec = P(('rep', 'ep'), None, 'tp', None)
    expert_spec = P(('ep', 'tp'), None, None)
    layer = functools.partial(fused_layer, shards=mesh.shape['ep'] * mesh.shape['tp'])
    in_specs = (tok_spec, P(None), P(None, 'tp'), P(None, 'tp'), P(None, 'tp'), P('tp', None), cache_spec, cache_spec, P(('rep', 'ep')), P(None), P(None, 'tp'), P(None, 'tp'), P('tp', None), expert_spec, expert_spec, expert_spec, tok_spec, tok_spec)
    return jax.shard_map(layer, mesh=mesh, in_specs=in_specs, out_specs=tok_spec, check_vma=False)
```

```python
import functools

import jax
import jax.numpy as jnp
from jax import lax
from jax.experimental import pallas as pl
from jax.experimental.pallas import tpu as pltpu
from jax.sharding import PartitionSpec as P

EPS = 1e-6
TILE = 256
SLOT = 32
HEAD = 128
BATCH = 16
GROUP = 3
CHUNKS = 4
LAG1, LAG2, LAG3 = 1, 4, 7
MESH_ID = pl.DeviceIdType.MESH


def rms_norm(values, gain):
    return values * lax.rsqrt(jnp.mean(values * values, axis=-1, keepdims=True) + EPS) * gain


def layer_kernel(len_in, h_in, gain_a_in, gain_f_in, ids_in, gv_in, wq_ref, wk_ref, wv_ref, wo_ref, kc_ref, vc_ref,
                 wsg_ref, wsu_ref, wsd_ref, wg_ref, wu_ref, wd_ref, out_ref,
                 x_all, x_rows, act, place_t, slot_gate, place, y_parts, ring, down, attn_ref, attn_rx, attn_sum, y_norm, gates, gt_ref,
                 len_ref, h_ref, gain_a_ref, gain_f_ref, ids_ref, gv_ref, q_buf, k_buf, v_buf, o_buf, p_buf, o_rows, send1, recv1, send2, recv2, send3, recv3, keep_own, keep_other,
                 ring_sem, down_sem, kv_sem, w_sem, x_ssem, x_rsem, g_ssem, g_rsem, a_sem, s1_sem, r1_sem, s2_sem, r2_sem, s3_sem, r3_sem, in_sem):
    tp = lax.axis_index('tp')
    ep = lax.axis_index('ep')
    core = ep % 2
    chip = ep // 2
    mate = chip * 2 + 1 - core
    across = (1 - chip) * 2 + core
    diagonal = (1 - chip) * 2 + 1 - core
    tokens, d_model = h_ref.shape
    n_heads = wq_ref.shape[1] // HEAD
    n_kv = wk_ref.shape[1] // HEAD
    group = n_heads // n_kv
    ctx_rows = kc_ref.shape[1] // 2
    x_ref = x_all.at[ep]
    n_local, _, hidden_dim = wg_ref.shape
    n_tiles = d_model // TILE

    def expert_copies(j, slot):
        return (pltpu.make_async_copy(wg_ref.at[j], ring.at[slot, 0], ring_sem.at[slot, 0]),
                pltpu.make_async_copy(wu_ref.at[j], ring.at[slot, 1], ring_sem.at[slot, 1]))

    def shared_copies(slot):
        return (pltpu.make_async_copy(wsg_ref, ring.at[slot, 0], ring_sem.at[slot, 0]),
                pltpu.make_async_copy(wsu_ref, ring.at[slot, 1], ring_sem.at[slot, 1]))

    def down_copies(i, slot):
        cols = pl.ds(pl.multiple_of(i * TILE, TILE), TILE)
        base = slot * (n_local + 1)
        parts = [(j, min(GROUP, n_local - j)) for j in range(0, n_local, GROUP)]
        copies = [[pltpu.make_async_copy(wd_ref.at[pl.ds(j, n), :, cols], down.at[pl.ds(base + j, n)], down_sem.at[slot, k])] for k, (j, n) in enumerate(parts)]
        copies[-1].append(pltpu.make_async_copy(wsd_ref.at[:, cols], down.at[base + n_local], down_sem.at[slot, len(parts)]))
        return copies

    def down_start(i, slot):
        for part in down_copies(i, slot):
            start(part)

    def cache_copies(i, n):
        slot = i % 2
        pairs = BATCH // 2
        copies = []
        for k in range(pairs):
            dst = down.at[slot * pairs + k, pl.ds(0, 2 * ctx_rows)]
            copies.append(pltpu.make_async_copy((kc_ref, vc_ref)[n].at[i * pairs + k], dst.at[:, pl.ds(n * HEAD, HEAD)], kv_sem.at[slot, k, n]))
        return copies

    def start(copies):
        for c in copies:
            c.start()

    def wait(copies):
        for c in copies:
            c.wait()

    qw, kvw = n_heads * HEAD, n_kv * HEAD
    proj = (pltpu.make_async_copy(wq_ref, ring.at[0, 0, :, pl.ds(0, qw)], w_sem.at[0]),
            pltpu.make_async_copy(wk_ref, ring.at[0, 1, :, pl.ds(0, kvw)], w_sem.at[1]),
            pltpu.make_async_copy(wv_ref, ring.at[0, 1, :, pl.ds(kvw, kvw)], w_sem.at[2]))
    out_proj = pltpu.make_async_copy(wo_ref, x_rows, w_sem.at[3])
    small = [pltpu.make_async_copy(src, dst, in_sem.at[k]) for k, (src, dst) in enumerate(
        ((h_in, h_ref), (gain_a_in, gain_a_ref), (ids_in, ids_ref), (gv_in, gv_ref), (len_in, len_ref), (gain_f_in, gain_f_ref)))]
    start(small)
    start(proj)
    for i in range(2):
        start(cache_copies(i, 0))
        start(cache_copies(i, 1))
    out_proj.start()

    barrier = pltpu.get_barrier_semaphore()
    for dev in ({'ep': mate}, {'ep': across}, {'ep': diagonal}, {'tp': 1 - tp}):
        pl.semaphore_signal(barrier, inc=1, device_id=dev, device_id_type=MESH_ID)

    wait(small)
    block_rows = 16
    expert_row = lax.broadcasted_iota(jnp.int32, gt_ref.shape, 0)
    table = jnp.zeros(gt_ref.shape, jnp.float32)
    for j in range(ids_ref.shape[0]):
        table = table + jnp.where(ids_ref[j:j + 1, :] == expert_row, gv_ref[j:j + 1, :], 0.0)
    gt_ref[...] = table

    def attn_norm(r, carry):
        rows = pl.ds(pl.multiple_of(r * block_rows, block_rows), block_rows)
        x_ref[rows, :] = rms_norm(h_ref[rows, :].astype(jnp.float32), gain_a_ref[...]).astype(jnp.bfloat16)
        return carry

    pl.semaphore_wait(barrier, 4)

    def recv_wait(dst, sem):
        pltpu.make_async_copy(dst, dst, sem).wait()

    def remote(src, dst, ssem, rsem, dev):
        return pltpu.make_async_remote_copy(src_ref=src, dst_ref=dst, send_sem=ssem, recv_sem=rsem, device_id=dev, device_id_type=MESH_ID)

    def gate_rows(shard):
        return gt_ref.at[pl.ds(pl.multiple_of((shard * 2 + tp) * n_local, n_local), n_local)]

    g_sends = [remote(gate_rows(peer), gates.at[ep], g_ssem.at[k], g_rsem.at[ep], {'ep': peer}) for k, peer in enumerate((mate, across, diagonal))]
    chunk_rows = tokens // CHUNKS

    def chunk(src, c):
        return x_all.at[src, pl.ds(c * chunk_rows, chunk_rows)]

    def x_recv(src):
        for c in range(CHUNKS):
            recv_wait(chunk(src, c), x_rsem.at[src, c])

    x_sends = [[remote(chunk(ep, c), chunk(ep, c), x_ssem.at[k, c], x_rsem.at[ep, c], {'ep': peer}) for k, peer in enumerate((across, mate))] for c in range(CHUNKS)]
    x_fwd = [remote(chunk(across, c), chunk(across, c), x_ssem.at[2, c], x_rsem.at[across, c], {'ep': mate}) for c in range(CHUNKS)]
    a_send = remote(attn_ref, attn_rx, a_sem.at[0], a_sem.at[1], {'tp': 1 - tp})
    start(g_sends)
    blocks = chunk_rows // block_rows
    for c in range(CHUNKS):
        lax.fori_loop(c * blocks, (c + 1) * blocks, attn_norm, 0, unroll=True)
        start(x_sends[c])

    def forward(c):
        recv_wait(chunk(across, c), x_rsem.at[across, c])
        x_fwd[c].start()

    lane = lax.broadcasted_iota(jnp.int32, (tokens, tokens), 1)
    row = lax.broadcasted_iota(jnp.int32, (tokens, tokens), 0)
    before = (row < lane).astype(jnp.bfloat16)
    slot_row = lax.broadcasted_iota(jnp.int32, (SLOT, tokens), 0).astype(jnp.float32)

    def dispatch(s, block):
        rows = pl.ds(pl.multiple_of(s * SLOT, SLOT), SLOT)
        gate = gates[s]
        chosen = (gate > 0.0).astype(jnp.float32)
        pos = jnp.dot(chosen.astype(jnp.bfloat16), before, preferred_element_type=jnp.float32)
        for j in range(n_local):
            hit = (pos[j:j + 1, :] == slot_row) & (chosen[j:j + 1, :] > 0.0)
            place[j * SLOT:(j + 1) * SLOT, :] = jnp.where(hit, 1.0, 0.0)
            picked = jnp.sum(jnp.where(hit, gate[j:j + 1, :], 0.0), axis=-1, keepdims=True)
            slot_gate[j, rows, :] = jnp.broadcast_to(picked, (SLOT, tokens))
        placed = place[...]
        place_t[s] = placed.T.astype(jnp.bfloat16)
        placed = placed.astype(jnp.bfloat16)

        for n in range(n_tiles):
            cols = slice(n * TILE, (n + 1) * TILE)
            got = jnp.dot(placed, block[:, cols], preferred_element_type=jnp.float32).astype(jnp.bfloat16)
            x_rows[:, rows, cols] = got.reshape(n_local, SLOT, TILE)

    x_own = x_ref[...]
    wait(proj)
    for n in range(qw // TILE):
        got = jnp.dot(x_own, ring[0, 0, :, n * TILE:(n + 1) * TILE], preferred_element_type=jnp.float32).astype(jnp.bfloat16).astype(jnp.float32)
        for k in range(TILE // HEAD):
            q_buf[:, n * (TILE // HEAD) + k, :] = got[:, k * HEAD:(k + 1) * HEAD]
    for n, buf in enumerate((k_buf, v_buf)):
        got = jnp.dot(x_own, ring[0, 1, :, n * kvw:(n + 1) * kvw], preferred_element_type=jnp.float32).astype(jnp.bfloat16).astype(jnp.float32)
        for k in range(n_heads):
            buf[:, k, :] = got[:, (k // group) * HEAD:(k // group + 1) * HEAD]

    scale = HEAD ** -0.5
    cache_lane = lax.broadcasted_iota(jnp.int32, (n_heads, ctx_rows), 1)
    head_row = lax.broadcasted_iota(jnp.int32, (n_heads, ctx_rows), 0)
    cache_pos = jnp.where(cache_lane % n_kv == head_row // group, cache_lane // n_kv, ctx_rows)

    def attend(i, carry):
        for c in range(CHUNKS // 2):
            @pl.when(i == n_batches - CHUNKS // 2 + c)
            def _(c=c):
                forward(c)

        first = i * BATCH
        base = (i % 2) * (BATCH // 2)
        wait(cache_copies(i, 0))

        def cache(u, n):
            return down[base + u // 2, (u % 2) * ctx_rows:(u % 2 + 1) * ctx_rows, n * HEAD:(n + 1) * HEAD]

        q_all = q_buf[pl.ds(pl.multiple_of(first, BATCH), BATCH)].reshape(BATCH * n_heads, HEAD).astype(jnp.bfloat16)
        stats = []
        for u in range(BATCH):
            t = first + u
            own_rows = slice(u * n_heads, (u + 1) * n_heads)
            s = lax.dot_general(q_all, cache(u, 0), (((1,), (1,)), ((), ())), preferred_element_type=jnp.float32)[own_rows] * scale
            s = jnp.where(cache_pos < len_ref[t], s, -jnp.inf)
            own = jnp.sum(q_buf[t] * k_buf[t], axis=-1, keepdims=True) * scale
            top = jnp.maximum(jnp.max(s, axis=-1, keepdims=True), own)
            w = jnp.exp(s - top)
            w_own = jnp.exp(own - top)
            p_buf[own_rows, :] = w
            stats.append((w_own, jnp.sum(w, axis=-1, keepdims=True) + w_own))

        @pl.when(i + 2 < n_batches)
        def _():
            start(cache_copies(i + 2, 0))

        wait(cache_copies(i, 1))
        p_all = p_buf[...].astype(jnp.bfloat16)
        for u in range(0, BATCH, 2):
            pair = jnp.concatenate([cache(u, 1), cache(u + 1, 1)], axis=1)
            mixed = jnp.dot(p_all, pair, preferred_element_type=jnp.float32)
            for e in range(2):
                w_own, norm = stats[u + e]
                mine = mixed[(u + e) * n_heads:(u + e + 1) * n_heads, e * HEAD:(e + 1) * HEAD]
                t = first + u + e
                o_buf[t] = (mine + w_own.astype(jnp.bfloat16).astype(jnp.float32) * v_buf[t]) / norm

        @pl.when(i + 2 < n_batches)
        def _():
            start(cache_copies(i + 2, 1))

        @pl.when(i == n_batches - 3)
        def _():
            start(expert_copies(0, 0))
            start(expert_copies(1, 1))
        return carry
    n_batches = tokens // BATCH
    lax.fori_loop(0, n_batches, attend, 0)
    down_start(0, 0)

    for k in range(n_heads):
        o_rows[:, k * HEAD:(k + 1) * HEAD] = o_buf[:, k, :].astype(jnp.bfloat16)
    out_proj.wait()
    for n in range(n_tiles):
        cols = slice(n * TILE, (n + 1) * TILE)
        got = jnp.dot(o_rows[...], x_rows[:, :, cols].reshape(qw, TILE), preferred_element_type=jnp.float32)
        attn_ref[:, cols] = got.astype(jnp.bfloat16)

    for c in range(CHUNKS // 2, CHUNKS):
        forward(c)

    gates[ep] = gt_ref[pl.ds(pl.multiple_of((ep * 2 + tp) * n_local, n_local), n_local), :]
    dispatch(ep, x_ref)
    for src in (mate, across, diagonal):
        recv_wait(gates.at[src], g_rsem.at[src])
    x_recv(mate)
    dispatch(mate, x_all.at[mate])
    a_send.start()
    dispatch(across, x_all.at[across])
    x_recv(diagonal)
    dispatch(diagonal, x_all.at[diagonal])

    def gate_up(lhs, slot, dst):
        full = hidden_dim // TILE * TILE
        for c in range(0, full, TILE):
            cols = slice(c, c + TILE)
            g = jnp.dot(lhs[...], ring[slot, 0, :, cols], preferred_element_type=jnp.float32)
            u = jnp.dot(lhs[...], ring[slot, 1, :, cols], preferred_element_type=jnp.float32)
            act[dst, :, cols] = (jax.nn.silu(g) * u).astype(jnp.bfloat16)
        if full < hidden_dim:
            cols = slice(full, hidden_dim)
            both = jnp.concatenate([ring[slot, 0, :, cols], ring[slot, 1, :, cols]], axis=1)
            gu = jnp.dot(lhs[...], both, preferred_element_type=jnp.float32)
            rest = hidden_dim - full
            act[dst, :, cols] = (jax.nn.silu(gu[:, :rest]) * gu[:, rest:]).astype(jnp.bfloat16)

    def expert(j, carry):
        slot = j % 2
        wait(expert_copies(j, slot))
        gate_up(x_rows.at[j], slot, j)

        @pl.when(j + 2 < n_local)
        def _():
            start(expert_copies(j + 2, slot))

        @pl.when(j + 2 == n_local)
        def _():
            start(shared_copies(slot))
        return carry
    lax.fori_loop(0, n_local, expert, 0)
    shared_slot = n_local % 2
    down_start(1, 1)

    recv_wait(attn_rx, a_sem.at[1])

    def ffn_norm(r, carry):
        rows = pl.ds(pl.multiple_of(r * block_rows, block_rows), block_rows)
        attn = (attn_ref[rows, :].astype(jnp.float32) + attn_rx[rows, :].astype(jnp.float32)).astype(jnp.bfloat16).astype(jnp.float32)
        res = h_ref[rows, :].astype(jnp.float32) + attn
        attn_sum[rows, :] = res
        y_norm[rows, :] = rms_norm(res, gain_f_ref[...]).astype(jnp.bfloat16)
        return carry
    lax.fori_loop(0, tokens // block_rows, ffn_norm, 0, unroll=4)
    wait(shared_copies(shared_slot))
    gate_up(y_norm, shared_slot, n_local)

    def split3(v):
        a = v.astype(jnp.bfloat16)
        r = v - a.astype(jnp.float32)
        b = r.astype(jnp.bfloat16)
        c = (r - b.astype(jnp.float32)).astype(jnp.bfloat16)
        return a, b, c

    def combine(s):
        rows = pl.ds(pl.multiple_of(s * SLOT, SLOT), SLOT)
        sums = [jnp.dot(place_t[s], y_parts[p, :, rows, :].reshape(n_local * SLOT, TILE), preferred_element_type=jnp.float32) for p in range(3)]
        return sums[0] + (sums[1] + sums[2])

    def s1_copy(i):
        return remote(send1.at[i], recv1.at[i], s1_sem.at[i], r1_sem.at[i], {'ep': mate})

    def s2_copy(i):
        return remote(send2.at[i], recv2.at[i], s2_sem.at[i], r2_sem.at[i], {'ep': across})

    def s3_copy(i):
        return remote(send3.at[i], recv3.at[i], s3_sem.at[i], r3_sem.at[i], {'tp': 1 - tp})

    def down_tile(i, slot):
        base = slot * (n_local + 1)
        now, later = down_copies(i, slot), down_copies(i + 2, slot)
        for k in range(len(now)):
            wait(now[k])
            for j in range(k * GROUP, min((k + 1) * GROUP, n_local)):
                out = jnp.dot(act[j], down[base + j], preferred_element_type=jnp.float32)
                parts = split3(out * jnp.concatenate([slot_gate[j]] * (TILE // tokens), axis=-1))
                for p in range(3):
                    y_parts[p, j] = parts[p]
            if k == len(now) - 1:
                keep_own[i] = jnp.dot(act[n_local], down[base + n_local], preferred_element_type=jnp.float32)

            @pl.when(i + 2 < n_tiles)
            def _(k=k):
                start(later[k])
        for b in range(2):
            send1[i, b] = combine(b * 2 + 1 - core).astype(jnp.bfloat16)
        s1_copy(i).start()
        keep_other[i] = combine((1 - chip) * 2 + core)
        keep_own[i] = keep_own[i] + combine(ep)

    def step(i, carry):
        @pl.when(i < n_tiles)
        def _():
            down_tile(i, i % 2)

        @pl.when((i >= LAG1) & (i < n_tiles + LAG1))
        def _():
            k = i - LAG1
            recv_wait(recv1.at[k], r1_sem.at[k])
            send2[k] = (keep_other[k] + recv1[k, 1 - chip].astype(jnp.float32)).astype(jnp.bfloat16)
            s2_copy(k).start()
            keep_own[k] = keep_own[k] + recv1[k, chip].astype(jnp.float32)

        @pl.when((i >= LAG2) & (i < n_tiles + LAG2))
        def _():
            k = i - LAG2
            recv_wait(recv2.at[k], r2_sem.at[k])
            send3[k] = (keep_own[k] + recv2[k].astype(jnp.float32)).astype(jnp.bfloat16)
            s3_copy(k).start()

        @pl.when(i >= LAG3)
        def _():
            k = i - LAG3
            cols = pl.ds(pl.multiple_of(k * TILE, TILE), TILE)
            recv_wait(recv3.at[k], r3_sem.at[k])
            ffn = send3[k].astype(jnp.float32) + recv3[k].astype(jnp.float32)
            out_ref[:, cols] = (attn_sum[:, cols] + ffn).astype(jnp.bfloat16)
        return carry
    lax.fori_loop(0, n_tiles + LAG3, step, 0)

    for c in g_sends + sum(x_sends, x_fwd) + [a_send]:
        c.wait_send()

    def drain(i, carry):
        s1_copy(i).wait_send()
        s2_copy(i).wait_send()
        s3_copy(i).wait_send()
        return carry
    lax.fori_loop(0, n_tiles, drain, 0)


def fused_layer(hidden, g_attn, w_q, w_k, w_v, w_o, k_cache, v_cache, lengths, g_ffn, ws_gate, ws_up, ws_down, w_gate, w_up, w_down, expert_ids, gate_vals, shards):
    tokens, d_model = hidden.shape
    n_local, _, hidden_dim = w_gate.shape
    n_tiles = d_model // TILE
    n_heads = w_q.shape[1] // HEAD
    ctx_len, n_kv = k_cache.shape[1:3]
    bf16, f32 = jnp.bfloat16, jnp.float32
    dma = pltpu.SemaphoreType.DMA
    hbm = pl.BlockSpec(memory_space=pltpu.HBM)
    tile = pltpu.VMEM((n_tiles, tokens, TILE), bf16)
    tile_f32 = pltpu.VMEM((n_tiles, tokens, TILE), f32)
    pair_tile = pltpu.VMEM((n_tiles, 2, tokens, TILE), bf16)
    rows_bf16 = pltpu.VMEM((tokens, d_model), bf16)
    heads = pltpu.VMEM((tokens, n_heads, HEAD), f32)
    caches = [c.reshape(tokens // 2, 2 * ctx_len * n_kv, HEAD) for c in (k_cache, v_cache)]
    return pl.pallas_call(
        layer_kernel,
        out_shape=pltpu.VMEM((tokens, d_model), bf16),
        in_specs=[hbm] * 18,
        out_specs=pl.BlockSpec(memory_space=pltpu.VMEM),
        scratch_shapes=[
            pltpu.VMEM((4, tokens, d_model), bf16),
            pltpu.VMEM((n_local, 4 * SLOT, d_model), bf16),
            pltpu.VMEM((n_local + 1, tokens, hidden_dim), bf16),
            pltpu.VMEM((4, tokens, n_local * SLOT), bf16),
            pltpu.VMEM((n_local, 4 * SLOT, tokens), f32),
            pltpu.VMEM((n_local * SLOT, tokens), f32),
            pltpu.VMEM((3, n_local, 4 * SLOT, TILE), bf16),
            pltpu.VMEM((2, 2, d_model, hidden_dim), bf16),
            pltpu.VMEM((2 * (n_local + 1), hidden_dim, TILE), bf16),
            rows_bf16, rows_bf16,
            pltpu.VMEM((tokens, d_model), f32),
            rows_bf16,
            pltpu.VMEM((4, n_local, tokens), f32),
            pltpu.VMEM((n_local * shards, tokens), f32),
            pltpu.SMEM((tokens,), jnp.int32), rows_bf16, pltpu.VMEM((1, d_model), f32), pltpu.VMEM((1, d_model), f32),
            pltpu.VMEM(expert_ids.shape[::-1], jnp.int32), pltpu.VMEM(gate_vals.shape[::-1], f32),
            heads, heads, heads, heads,
            pltpu.VMEM((BATCH * n_heads, ctx_len * n_kv), f32),
            pltpu.VMEM((tokens, n_heads * HEAD), bf16),
            pair_tile, pair_tile, tile, tile, tile, tile, tile_f32, tile_f32,
            dma((2, 2)), dma((2, 4)), dma((2, BATCH // 2, 2)), dma((4,)), dma((3, CHUNKS)), dma((4, CHUNKS)), dma((3,)), dma((4,)), dma((2,)),
        ] + [dma((n_tiles,))] * 6 + [dma((6,))],
        compiler_params=pltpu.CompilerParams(collective_id=0, has_side_effects=True, vmem_limit_bytes=63 * 1024 * 1024),
        cost_estimate=pl.CostEstimate(flops=2 * tokens * (n_local + 1) * 3 * d_model * hidden_dim, bytes_accessed=(n_local + 1) * 6 * d_model * hidden_dim, transcendentals=0),
        name='layer',
    )(lengths, hidden, g_attn.reshape(1, d_model), g_ffn.reshape(1, d_model), expert_ids.T, gate_vals.T, w_q, w_k, w_v, w_o.reshape(n_heads, HEAD, d_model), *caches, ws_gate, ws_up, ws_down, w_gate, w_up, w_down)


def solution(mesh):
    tok_spec = P(('rep', 'ep'), None)
    cache_spec = P(('rep', 'ep'), None, 'tp', None)
    expert_spec = P(('ep', 'tp'), None, None)
    layer = functools.partial(fused_layer, shards=mesh.shape['ep'] * mesh.shape['tp'])
    in_specs = (tok_spec, P(None), P(None, 'tp'), P(None, 'tp'), P(None, 'tp'), P('tp', None), cache_spec, cache_spec, P(('rep', 'ep')), P(None), P(None, 'tp'), P(None, 'tp'), P('tp', None), expert_spec, expert_spec, expert_spec, tok_spec, tok_spec)
    return jax.shard_map(layer, mesh=mesh, in_specs=in_specs, out_specs=tok_spec, check_vma=False)
```

```python
import functools

import jax
import jax.numpy as jnp
from jax import lax
from jax.experimental import pallas as pl
from jax.experimental.pallas import tpu as pltpu
from jax.sharding import PartitionSpec as P

EPS = 1e-6
TILE = 256
SLOT = 32
HEAD = 128
BATCH = 16
GROUP = 3
CHUNKS = 4
LAG1, LAG2, LAG3 = 1, 4, 7
MESH_ID = pl.DeviceIdType.MESH


def rms_norm(values, gain):
    return values * lax.rsqrt(jnp.mean(values * values, axis=-1, keepdims=True) + EPS) * gain


def layer_kernel(len_in, h_in, gain_a_in, gain_f_in, ids_in, gv_in, wq_ref, wk_ref, wv_ref, wo_ref, kc_ref, vc_ref,
                 wsg_ref, wsu_ref, wsd_ref, wg_ref, wu_ref, wd_ref, out_ref,
                 x_all, x_rows, act, place_t, slot_gate, place, y_parts, ring, down, attn_ref, attn_rx, attn_sum, y_norm, gates, gt_ref,
                 len_ref, h_ref, gain_a_ref, gain_f_ref, ids_ref, gv_ref, q_buf, k_buf, v_buf, o_buf, p_buf, o_rows, send1, recv1, send2, recv2, send3, recv3, keep_own, keep_other,
                 ring_sem, down_sem, kv_sem, w_sem, x_ssem, x_rsem, g_ssem, g_rsem, a_sem, s1_sem, r1_sem, s2_sem, r2_sem, s3_sem, r3_sem, in_sem):
    tp = lax.axis_index('tp')
    ep = lax.axis_index('ep')
    core = ep % 2
    chip = ep // 2
    mate = chip * 2 + 1 - core
    across = (1 - chip) * 2 + core
    diagonal = (1 - chip) * 2 + 1 - core
    tokens, d_model = h_ref.shape
    n_heads = wq_ref.shape[1] // HEAD
    n_kv = wk_ref.shape[1] // HEAD
    group = n_heads // n_kv
    ctx_rows = kc_ref.shape[1] // 2
    x_ref = x_all.at[ep]
    n_local, _, hidden_dim = wg_ref.shape
    n_tiles = d_model // TILE

    def expert_copies(j, slot):
        return (pltpu.make_async_copy(wg_ref.at[j], ring.at[slot, 0], ring_sem.at[slot, 0]),
                pltpu.make_async_copy(wu_ref.at[j], ring.at[slot, 1], ring_sem.at[slot, 1]))

    def shared_copies(slot):
        return (pltpu.make_async_copy(wsg_ref, ring.at[slot, 0], ring_sem.at[slot, 0]),
                pltpu.make_async_copy(wsu_ref, ring.at[slot, 1], ring_sem.at[slot, 1]))

    def down_copies(i, slot):
        cols = pl.ds(pl.multiple_of(i * TILE, TILE), TILE)
        base = slot * (n_local + 1)
        parts = [(j, min(GROUP, n_local - j)) for j in range(0, n_local, GROUP)]
        copies = [[pltpu.make_async_copy(wd_ref.at[pl.ds(j, n), :, cols], down.at[pl.ds(base + j, n)], down_sem.at[slot, k])] for k, (j, n) in enumerate(parts)]
        copies[-1].append(pltpu.make_async_copy(wsd_ref.at[:, cols], down.at[base + n_local], down_sem.at[slot, len(parts)]))
        return copies

    def down_start(i, slot):
        for part in down_copies(i, slot):
            start(part)

    def cache_copies(i, n):
        slot = i % 2
        pairs = BATCH // 2
        copies = []
        for k in range(pairs):
            dst = down.at[slot * pairs + k, pl.ds(0, 2 * ctx_rows)]
            copies.append(pltpu.make_async_copy((kc_ref, vc_ref)[n].at[i * pairs + k], dst.at[:, pl.ds(n * HEAD, HEAD)], kv_sem.at[slot, k, n]))
        return copies

    def start(copies):
        for c in copies:
            c.start()

    def wait(copies):
        for c in copies:
            c.wait()

    qw, kvw = n_heads * HEAD, n_kv * HEAD
    proj = (pltpu.make_async_copy(wq_ref, ring.at[0, 0, :, pl.ds(0, qw)], w_sem.at[0]),
            pltpu.make_async_copy(wk_ref, ring.at[0, 1, :, pl.ds(0, kvw)], w_sem.at[1]),
            pltpu.make_async_copy(wv_ref, ring.at[0, 1, :, pl.ds(kvw, kvw)], w_sem.at[2]))
    out_proj = pltpu.make_async_copy(wo_ref, x_rows, w_sem.at[3])
    small = [pltpu.make_async_copy(src, dst, in_sem.at[k]) for k, (src, dst) in enumerate(
        ((h_in, h_ref), (gain_a_in, gain_a_ref), (ids_in, ids_ref), (gv_in, gv_ref), (len_in, len_ref), (gain_f_in, gain_f_ref)))]
    start(small)
    start(proj)
    for i in range(2):
        start(cache_copies(i, 0))
        start(cache_copies(i, 1))
    out_proj.start()

    barrier = pltpu.get_barrier_semaphore()
    for dev in ({'ep': mate}, {'ep': across}, {'ep': diagonal}, {'tp': 1 - tp}):
        pl.semaphore_signal(barrier, inc=1, device_id=dev, device_id_type=MESH_ID)

    wait(small)
    block_rows = 16
    expert_row = lax.broadcasted_iota(jnp.int32, gt_ref.shape, 0)
    table = jnp.zeros(gt_ref.shape, jnp.float32)
    for j in range(ids_ref.shape[0]):
        table = table + jnp.where(ids_ref[j:j + 1, :] == expert_row, gv_ref[j:j + 1, :], 0.0)
    gt_ref[...] = table

    def attn_norm(r, carry):
        rows = pl.ds(pl.multiple_of(r * block_rows, block_rows), block_rows)
        x_ref[rows, :] = rms_norm(h_ref[rows, :].astype(jnp.float32), gain_a_ref[...]).astype(jnp.bfloat16)
        return carry

    pl.semaphore_wait(barrier, 4)

    def recv_wait(dst, sem):
        pltpu.make_async_copy(dst, dst, sem).wait()

    def remote(src, dst, ssem, rsem, dev):
        return pltpu.make_async_remote_copy(src_ref=src, dst_ref=dst, send_sem=ssem, recv_sem=rsem, device_id=dev, device_id_type=MESH_ID)

    def gate_rows(shard):
        return gt_ref.at[pl.ds(pl.multiple_of((shard * 2 + tp) * n_local, n_local), n_local)]

    g_sends = [remote(gate_rows(peer), gates.at[ep], g_ssem.at[k], g_rsem.at[ep], {'ep': peer}) for k, peer in enumerate((mate, across, diagonal))]
    chunk_rows = tokens // CHUNKS

    def chunk(src, c):
        return x_all.at[src, pl.ds(c * chunk_rows, chunk_rows)]

    def x_recv(src):
        for c in range(CHUNKS):
            recv_wait(chunk(src, c), x_rsem.at[src, c])

    x_sends = [[remote(chunk(ep, c), chunk(ep, c), x_ssem.at[k, c], x_rsem.at[ep, c], {'ep': peer}) for k, peer in enumerate((across, mate))] for c in range(CHUNKS)]
    x_fwd = [remote(chunk(across, c), chunk(across, c), x_ssem.at[2, c], x_rsem.at[across, c], {'ep': mate}) for c in range(CHUNKS)]
    a_send = remote(attn_ref, attn_rx, a_sem.at[0], a_sem.at[1], {'tp': 1 - tp})
    start(g_sends)
    blocks = chunk_rows // block_rows
    for c in range(CHUNKS):
        lax.fori_loop(c * blocks, (c + 1) * blocks, attn_norm, 0, unroll=True)
        start(x_sends[c])

    def forward(c):
        recv_wait(chunk(across, c), x_rsem.at[across, c])
        x_fwd[c].start()

    lane = lax.broadcasted_iota(jnp.int32, (tokens, tokens), 1)
    row = lax.broadcasted_iota(jnp.int32, (tokens, tokens), 0)
    before = (row < lane).astype(jnp.bfloat16)
    slot_row = lax.broadcasted_iota(jnp.int32, (SLOT, tokens), 0).astype(jnp.float32)

    def dispatch(s, block):
        rows = pl.ds(pl.multiple_of(s * SLOT, SLOT), SLOT)
        gate = gates[s]
        chosen = (gate > 0.0).astype(jnp.float32)
        pos = jnp.dot(chosen.astype(jnp.bfloat16), before, preferred_element_type=jnp.float32)
        for j in range(n_local):
            hit = (pos[j:j + 1, :] == slot_row) & (chosen[j:j + 1, :] > 0.0)
            place[j * SLOT:(j + 1) * SLOT, :] = jnp.where(hit, 1.0, 0.0)
            picked = jnp.sum(jnp.where(hit, gate[j:j + 1, :], 0.0), axis=-1, keepdims=True)
            slot_gate[j, rows, :] = jnp.broadcast_to(picked, (SLOT, tokens))
        placed = place[...]
        place_t[s] = placed.T.astype(jnp.bfloat16)
        placed = placed.astype(jnp.bfloat16)

        for n in range(n_tiles):
            cols = slice(n * TILE, (n + 1) * TILE)
            got = jnp.dot(placed, block[:, cols], preferred_element_type=jnp.float32).astype(jnp.bfloat16)
            x_rows[:, rows, cols] = got.reshape(n_local, SLOT, TILE)

    x_own = x_ref[...]
    wait(proj)
    for n in range(qw // TILE):
        got = jnp.dot(x_own, ring[0, 0, :, n * TILE:(n + 1) * TILE], preferred_element_type=jnp.float32).astype(jnp.bfloat16).astype(jnp.float32)
        for k in range(TILE // HEAD):
            q_buf[:, n * (TILE // HEAD) + k, :] = got[:, k * HEAD:(k + 1) * HEAD]
    for n, buf in enumerate((k_buf, v_buf)):
        got = jnp.dot(x_own, ring[0, 1, :, n * kvw:(n + 1) * kvw], preferred_element_type=jnp.float32).astype(jnp.bfloat16).astype(jnp.float32)
        for k in range(n_heads):
            buf[:, k, :] = got[:, (k // group) * HEAD:(k // group + 1) * HEAD]

    scale = HEAD ** -0.5
    cache_lane = lax.broadcasted_iota(jnp.int32, (n_heads, ctx_rows), 1)
    head_row = lax.broadcasted_iota(jnp.int32, (n_heads, ctx_rows), 0)
    cache_pos = jnp.where(cache_lane % n_kv == head_row // group, cache_lane // n_kv, ctx_rows)

    def attend(i, carry):
        for c in range(CHUNKS // 2):
            @pl.when(i == n_batches - CHUNKS // 2 + c)
            def _(c=c):
                forward(c)

        first = i * BATCH
        base = (i % 2) * (BATCH // 2)
        wait(cache_copies(i, 0))

        def cache(u, n):
            return down[base + u // 2, (u % 2) * ctx_rows:(u % 2 + 1) * ctx_rows, n * HEAD:(n + 1) * HEAD]

        q_all = q_buf[pl.ds(pl.multiple_of(first, BATCH), BATCH)].reshape(BATCH * n_heads, HEAD).astype(jnp.bfloat16)
        stats = []
        for u in range(BATCH):
            t = first + u
            own_rows = slice(u * n_heads, (u + 1) * n_heads)
            s = lax.dot_general(q_all, cache(u, 0), (((1,), (1,)), ((), ())), preferred_element_type=jnp.float32)[own_rows] * scale
            s = jnp.where(cache_pos < len_ref[t], s, -jnp.inf)
            own = jnp.sum(q_buf[t] * k_buf[t], axis=-1, keepdims=True) * scale
            top = jnp.maximum(jnp.max(s, axis=-1, keepdims=True), own)
            w = jnp.exp(s - top)
            w_own = jnp.exp(own - top)
            p_buf[own_rows, :] = w
            stats.append((w_own, jnp.sum(w, axis=-1, keepdims=True) + w_own))

        @pl.when(i + 2 < n_batches)
        def _():
            start(cache_copies(i + 2, 0))

        wait(cache_copies(i, 1))
        p_all = p_buf[...].astype(jnp.bfloat16)
        for u in range(0, BATCH, 2):
            pair = jnp.concatenate([cache(u, 1), cache(u + 1, 1)], axis=1)
            mixed = jnp.dot(p_all, pair, preferred_element_type=jnp.float32)
            for e in range(2):
                w_own, norm = stats[u + e]
                mine = mixed[(u + e) * n_heads:(u + e + 1) * n_heads, e * HEAD:(e + 1) * HEAD]
                t = first + u + e
                o_buf[t] = (mine + w_own.astype(jnp.bfloat16).astype(jnp.float32) * v_buf[t]) / norm

        @pl.when(i + 2 < n_batches)
        def _():
            start(cache_copies(i + 2, 1))

        @pl.when(i == n_batches - 3)
        def _():
            start(expert_copies(0, 0))
            start(expert_copies(1, 1))
        return carry
    n_batches = tokens // BATCH
    lax.fori_loop(0, n_batches, attend, 0)
    down_start(0, 0)

    for k in range(n_heads):
        o_rows[:, k * HEAD:(k + 1) * HEAD] = o_buf[:, k, :].astype(jnp.bfloat16)
    out_proj.wait()
    for n in range(n_tiles):
        cols = slice(n * TILE, (n + 1) * TILE)
        got = jnp.dot(o_rows[...], x_rows[:, :, cols].reshape(qw, TILE), preferred_element_type=jnp.float32)
        attn_ref[:, cols] = got.astype(jnp.bfloat16)

    gates[ep] = gt_ref[pl.ds(pl.multiple_of((ep * 2 + tp) * n_local, n_local), n_local), :]
    dispatch(ep, x_ref)
    for c in range(CHUNKS // 2, CHUNKS - 1):
        forward(c)
    for src in (mate, across, diagonal):
        recv_wait(gates.at[src], g_rsem.at[src])
    x_recv(mate)
    dispatch(mate, x_all.at[mate])
    forward(CHUNKS - 1)
    a_send.start()
    dispatch(across, x_all.at[across])
    x_recv(diagonal)
    dispatch(diagonal, x_all.at[diagonal])

    def gate_up(lhs, slot, dst):
        full = hidden_dim // TILE * TILE
        for c in range(0, full, TILE):
            cols = slice(c, c + TILE)
            g = jnp.dot(lhs[...], ring[slot, 0, :, cols], preferred_element_type=jnp.float32)
            u = jnp.dot(lhs[...], ring[slot, 1, :, cols], preferred_element_type=jnp.float32)
            act[dst, :, cols] = (jax.nn.silu(g) * u).astype(jnp.bfloat16)
        if full < hidden_dim:
            cols = slice(full, hidden_dim)
            both = jnp.concatenate([ring[slot, 0, :, cols], ring[slot, 1, :, cols]], axis=1)
            gu = jnp.dot(lhs[...], both, preferred_element_type=jnp.float32)
            rest = hidden_dim - full
            act[dst, :, cols] = (jax.nn.silu(gu[:, :rest]) * gu[:, rest:]).astype(jnp.bfloat16)

    def expert(j, carry):
        slot = j % 2
        wait(expert_copies(j, slot))
        gate_up(x_rows.at[j], slot, j)

        @pl.when(j + 2 < n_local)
        def _():
            start(expert_copies(j + 2, slot))

        @pl.when(j + 2 == n_local)
        def _():
            start(shared_copies(slot))
        return carry
    lax.fori_loop(0, n_local, expert, 0)
    shared_slot = n_local % 2
    down_start(1, 1)

    recv_wait(attn_rx, a_sem.at[1])

    def ffn_norm(r, carry):
        rows = pl.ds(pl.multiple_of(r * block_rows, block_rows), block_rows)
        attn = (attn_ref[rows, :].astype(jnp.float32) + attn_rx[rows, :].astype(jnp.float32)).astype(jnp.bfloat16).astype(jnp.float32)
        res = h_ref[rows, :].astype(jnp.float32) + attn
        attn_sum[rows, :] = res
        y_norm[rows, :] = rms_norm(res, gain_f_ref[...]).astype(jnp.bfloat16)
        return carry
    lax.fori_loop(0, tokens // block_rows, ffn_norm, 0, unroll=4)
    wait(shared_copies(shared_slot))
    gate_up(y_norm, shared_slot, n_local)

    def split3(v):
        a = v.astype(jnp.bfloat16)
        r = v - a.astype(jnp.float32)
        b = r.astype(jnp.bfloat16)
        c = (r - b.astype(jnp.float32)).astype(jnp.bfloat16)
        return a, b, c

    def combine(s):
        rows = pl.ds(pl.multiple_of(s * SLOT, SLOT), SLOT)
        sums = [jnp.dot(place_t[s], y_parts[p, :, rows, :].reshape(n_local * SLOT, TILE), preferred_element_type=jnp.float32) for p in range(3)]
        return sums[0] + (sums[1] + sums[2])

    def s1_copy(i):
        return remote(send1.at[i], recv1.at[i], s1_sem.at[i], r1_sem.at[i], {'ep': mate})

    def s2_copy(i):
        return remote(send2.at[i], recv2.at[i], s2_sem.at[i], r2_sem.at[i], {'ep': across})

    def s3_copy(i):
        return remote(send3.at[i], recv3.at[i], s3_sem.at[i], r3_sem.at[i], {'tp': 1 - tp})

    def down_tile(i, slot):
        base = slot * (n_local + 1)
        now, later = down_copies(i, slot), down_copies(i + 2, slot)
        for k in range(len(now)):
            wait(now[k])
            for j in range(k * GROUP, min((k + 1) * GROUP, n_local)):
                out = jnp.dot(act[j], down[base + j], preferred_element_type=jnp.float32)
                parts = split3(out * jnp.concatenate([slot_gate[j]] * (TILE // tokens), axis=-1))
                for p in range(3):
                    y_parts[p, j] = parts[p]
            if k == len(now) - 1:
                keep_own[i] = jnp.dot(act[n_local], down[base + n_local], preferred_element_type=jnp.float32)

            @pl.when(i + 2 < n_tiles)
            def _(k=k):
                start(later[k])
        for b in range(2):
            send1[i, b] = combine(b * 2 + 1 - core).astype(jnp.bfloat16)
        s1_copy(i).start()
        keep_other[i] = combine((1 - chip) * 2 + core)
        keep_own[i] = keep_own[i] + combine(ep)

    def step(i, carry):
        @pl.when(i < n_tiles)
        def _():
            down_tile(i, i % 2)

        @pl.when((i >= LAG1) & (i < n_tiles + LAG1))
        def _():
            k = i - LAG1
            recv_wait(recv1.at[k], r1_sem.at[k])
            send2[k] = (keep_other[k] + recv1[k, 1 - chip].astype(jnp.float32)).astype(jnp.bfloat16)
            s2_copy(k).start()
            keep_own[k] = keep_own[k] + recv1[k, chip].astype(jnp.float32)

        @pl.when((i >= LAG2) & (i < n_tiles + LAG2))
        def _():
            k = i - LAG2
            recv_wait(recv2.at[k], r2_sem.at[k])
            send3[k] = (keep_own[k] + recv2[k].astype(jnp.float32)).astype(jnp.bfloat16)
            s3_copy(k).start()

        @pl.when(i >= LAG3)
        def _():
            k = i - LAG3
            cols = pl.ds(pl.multiple_of(k * TILE, TILE), TILE)
            recv_wait(recv3.at[k], r3_sem.at[k])
            ffn = send3[k].astype(jnp.float32) + recv3[k].astype(jnp.float32)
            out_ref[:, cols] = (attn_sum[:, cols] + ffn).astype(jnp.bfloat16)
        return carry
    lax.fori_loop(0, n_tiles + LAG3, step, 0)

    for c in g_sends + sum(x_sends, x_fwd) + [a_send]:
        c.wait_send()

    def drain(i, carry):
        s1_copy(i).wait_send()
        s2_copy(i).wait_send()
        s3_copy(i).wait_send()
        return carry
    lax.fori_loop(0, n_tiles, drain, 0)


def fused_layer(hidden, g_attn, w_q, w_k, w_v, w_o, k_cache, v_cache, lengths, g_ffn, ws_gate, ws_up, ws_down, w_gate, w_up, w_down, expert_ids, gate_vals, shards):
    tokens, d_model = hidden.shape
    n_local, _, hidden_dim = w_gate.shape
    n_tiles = d_model // TILE
    n_heads = w_q.shape[1] // HEAD
    ctx_len, n_kv = k_cache.shape[1:3]
    bf16, f32 = jnp.bfloat16, jnp.float32
    dma = pltpu.SemaphoreType.DMA
    hbm = pl.BlockSpec(memory_space=pltpu.HBM)
    tile = pltpu.VMEM((n_tiles, tokens, TILE), bf16)
    tile_f32 = pltpu.VMEM((n_tiles, tokens, TILE), f32)
    pair_tile = pltpu.VMEM((n_tiles, 2, tokens, TILE), bf16)
    rows_bf16 = pltpu.VMEM((tokens, d_model), bf16)
    heads = pltpu.VMEM((tokens, n_heads, HEAD), f32)
    caches = [c.reshape(tokens // 2, 2 * ctx_len * n_kv, HEAD) for c in (k_cache, v_cache)]
    return pl.pallas_call(
        layer_kernel,
        out_shape=pltpu.VMEM((tokens, d_model), bf16),
        in_specs=[hbm] * 18,
        out_specs=pl.BlockSpec(memory_space=pltpu.VMEM),
        scratch_shapes=[
            pltpu.VMEM((4, tokens, d_model), bf16),
            pltpu.VMEM((n_local, 4 * SLOT, d_model), bf16),
            pltpu.VMEM((n_local + 1, tokens, hidden_dim), bf16),
            pltpu.VMEM((4, tokens, n_local * SLOT), bf16),
            pltpu.VMEM((n_local, 4 * SLOT, tokens), f32),
            pltpu.VMEM((n_local * SLOT, tokens), f32),
            pltpu.VMEM((3, n_local, 4 * SLOT, TILE), bf16),
            pltpu.VMEM((2, 2, d_model, hidden_dim), bf16),
            pltpu.VMEM((2 * (n_local + 1), hidden_dim, TILE), bf16),
            rows_bf16, rows_bf16,
            pltpu.VMEM((tokens, d_model), f32),
            rows_bf16,
            pltpu.VMEM((4, n_local, tokens), f32),
            pltpu.VMEM((n_local * shards, tokens), f32),
            pltpu.SMEM((tokens,), jnp.int32), rows_bf16, pltpu.VMEM((1, d_model), f32), pltpu.VMEM((1, d_model), f32),
            pltpu.VMEM(expert_ids.shape[::-1], jnp.int32), pltpu.VMEM(gate_vals.shape[::-1], f32),
            heads, heads, heads, heads,
            pltpu.VMEM((BATCH * n_heads, ctx_len * n_kv), f32),
            pltpu.VMEM((tokens, n_heads * HEAD), bf16),
            pair_tile, pair_tile, tile, tile, tile, tile, tile_f32, tile_f32,
            dma((2, 2)), dma((2, 4)), dma((2, BATCH // 2, 2)), dma((4,)), dma((3, CHUNKS)), dma((4, CHUNKS)), dma((3,)), dma((4,)), dma((2,)),
        ] + [dma((n_tiles,))] * 6 + [dma((6,))],
        compiler_params=pltpu.CompilerParams(collective_id=0, has_side_effects=True, vmem_limit_bytes=63 * 1024 * 1024),
        cost_estimate=pl.CostEstimate(flops=2 * tokens * (n_local + 1) * 3 * d_model * hidden_dim, bytes_accessed=(n_local + 1) * 6 * d_model * hidden_dim, transcendentals=0),
        name='layer',
    )(lengths, hidden, g_attn.reshape(1, d_model), g_ffn.reshape(1, d_model), expert_ids.T, gate_vals.T, w_q, w_k, w_v, w_o.reshape(n_heads, HEAD, d_model), *caches, ws_gate, ws_up, ws_down, w_gate, w_up, w_down)


def solution(mesh):
    tok_spec = P(('rep', 'ep'), None)
    cache_spec = P(('rep', 'ep'), None, 'tp', None)
    expert_spec = P(('ep', 'tp'), None, None)
    layer = functools.partial(fused_layer, shards=mesh.shape['ep'] * mesh.shape['tp'])
    in_specs = (tok_spec, P(None), P(None, 'tp'), P(None, 'tp'), P(None, 'tp'), P('tp', None), cache_spec, cache_spec, P(('rep', 'ep')), P(None), P(None, 'tp'), P(None, 'tp'), P('tp', None), expert_spec, expert_spec, expert_spec, tok_spec, tok_spec)
    return jax.shard_map(layer, mesh=mesh, in_specs=in_specs, out_specs=tok_spec, check_vma=False)
```

```python
import functools

import jax
import jax.numpy as jnp
from jax import lax
from jax.experimental import pallas as pl
from jax.experimental.pallas import tpu as pltpu
from jax.sharding import PartitionSpec as P

EPS = 1e-6
TILE = 256
SLOT = 32
HEAD = 128
BATCH = 16
GROUP = 3
CHUNKS = 4
LAG1, LAG2, LAG3 = 1, 4, 7
MESH_ID = pl.DeviceIdType.MESH


def rms_norm(values, gain):
    return values * lax.rsqrt(jnp.mean(values * values, axis=-1, keepdims=True) + EPS) * gain


def layer_kernel(len_in, h_in, gain_a_in, gain_f_in, ids_in, gv_in, wq_ref, wk_ref, wv_ref, wo_ref, kc_ref, vc_ref,
                 wsg_ref, wsu_ref, wsd_ref, wg_ref, wu_ref, wd_ref, out_ref,
                 x_all, x_rows, act, place_t, slot_gate, place, y_parts, ring, down, attn_ref, attn_rx, attn_sum, y_norm, gates, gt_ref,
                 len_ref, h_ref, gain_a_ref, gain_f_ref, ids_ref, gv_ref, q_buf, k_buf, v_buf, o_buf, p_buf, o_rows, send1, recv1, send2, recv2, send3, recv3, keep_own, keep_other,
                 ring_sem, down_sem, kv_sem, w_sem, x_ssem, x_rsem, g_ssem, g_rsem, a_sem, s1_sem, r1_sem, s2_sem, r2_sem, s3_sem, r3_sem, in_sem):
    tp = lax.axis_index('tp')
    ep = lax.axis_index('ep')
    core = ep % 2
    chip = ep // 2
    mate = chip * 2 + 1 - core
    across = (1 - chip) * 2 + core
    diagonal = (1 - chip) * 2 + 1 - core
    tokens, d_model = h_ref.shape
    n_heads = wq_ref.shape[1] // HEAD
    n_kv = wk_ref.shape[1] // HEAD
    group = n_heads // n_kv
    ctx_rows = kc_ref.shape[1] // 2
    x_ref = x_all.at[ep]
    n_local, _, hidden_dim = wg_ref.shape
    n_tiles = d_model // TILE

    def expert_copies(j, slot):
        return (pltpu.make_async_copy(wg_ref.at[j], ring.at[slot, 0], ring_sem.at[slot, 0]),
                pltpu.make_async_copy(wu_ref.at[j], ring.at[slot, 1], ring_sem.at[slot, 1]))

    def shared_copies(slot):
        return (pltpu.make_async_copy(wsg_ref, ring.at[slot, 0], ring_sem.at[slot, 0]),
                pltpu.make_async_copy(wsu_ref, ring.at[slot, 1], ring_sem.at[slot, 1]))

    def down_copies(i, slot):
        cols = pl.ds(pl.multiple_of(i * TILE, TILE), TILE)
        base = slot * (n_local + 1)
        parts = [(j, min(GROUP, n_local - j)) for j in range(0, n_local, GROUP)]
        copies = [[pltpu.make_async_copy(wd_ref.at[pl.ds(j, n), :, cols], down.at[pl.ds(base + j, n)], down_sem.at[slot, k])] for k, (j, n) in enumerate(parts)]
        copies[-1].append(pltpu.make_async_copy(wsd_ref.at[:, cols], down.at[base + n_local], down_sem.at[slot, len(parts)]))
        return copies

    def down_start(i, slot):
        for part in down_copies(i, slot):
            start(part)

    def cache_copies(i, n):
        slot = i % 2
        pairs = BATCH // 2
        copies = []
        for k in range(pairs):
            dst = down.at[slot * pairs + k, pl.ds(0, 2 * ctx_rows)]
            copies.append(pltpu.make_async_copy((kc_ref, vc_ref)[n].at[i * pairs + k], dst.at[:, pl.ds(n * HEAD, HEAD)], kv_sem.at[slot, k, n]))
        return copies

    def start(copies):
        for c in copies:
            c.start()

    def wait(copies):
        for c in copies:
            c.wait()

    qw, kvw = n_heads * HEAD, n_kv * HEAD
    proj = (pltpu.make_async_copy(wq_ref, ring.at[0, 0, :, pl.ds(0, qw)], w_sem.at[0]),
            pltpu.make_async_copy(wk_ref, ring.at[0, 1, :, pl.ds(0, kvw)], w_sem.at[1]),
            pltpu.make_async_copy(wv_ref, ring.at[0, 1, :, pl.ds(kvw, kvw)], w_sem.at[2]))
    out_proj = pltpu.make_async_copy(wo_ref, x_rows, w_sem.at[3])
    small = [pltpu.make_async_copy(src, dst, in_sem.at[k]) for k, (src, dst) in enumerate(
        ((h_in, h_ref), (gain_a_in, gain_a_ref), (ids_in, ids_ref), (gv_in, gv_ref), (len_in, len_ref), (gain_f_in, gain_f_ref)))]
    start(small)
    start(proj)
    for i in range(2):
        start(cache_copies(i, 0))
        start(cache_copies(i, 1))
    out_proj.start()

    barrier = pltpu.get_barrier_semaphore()
    for dev in ({'ep': mate}, {'ep': across}, {'ep': diagonal}, {'tp': 1 - tp}):
        pl.semaphore_signal(barrier, inc=1, device_id=dev, device_id_type=MESH_ID)

    wait(small)
    block_rows = 16
    expert_row = lax.broadcasted_iota(jnp.int32, gt_ref.shape, 0)
    table = jnp.zeros(gt_ref.shape, jnp.float32)
    for j in range(ids_ref.shape[0]):
        table = table + jnp.where(ids_ref[j:j + 1, :] == expert_row, gv_ref[j:j + 1, :], 0.0)
    gt_ref[...] = table

    def attn_norm(r, carry):
        rows = pl.ds(pl.multiple_of(r * block_rows, block_rows), block_rows)
        x_ref[rows, :] = rms_norm(h_ref[rows, :].astype(jnp.float32), gain_a_ref[...]).astype(jnp.bfloat16)
        return carry

    pl.semaphore_wait(barrier, 4)

    def recv_wait(dst, sem):
        pltpu.make_async_copy(dst, dst, sem).wait()

    def remote(src, dst, ssem, rsem, dev):
        return pltpu.make_async_remote_copy(src_ref=src, dst_ref=dst, send_sem=ssem, recv_sem=rsem, device_id=dev, device_id_type=MESH_ID)

    def gate_rows(shard):
        return gt_ref.at[pl.ds(pl.multiple_of((shard * 2 + tp) * n_local, n_local), n_local)]

    g_sends = [remote(gate_rows(peer), gates.at[ep], g_ssem.at[k], g_rsem.at[ep], {'ep': peer}) for k, peer in enumerate((mate, across, diagonal))]
    chunk_rows = tokens // CHUNKS

    def chunk(src, c):
        return x_all.at[src, pl.ds(c * chunk_rows, chunk_rows)]

    def x_recv(src):
        for c in range(CHUNKS):
            recv_wait(chunk(src, c), x_rsem.at[src, c])

    x_sends = [[remote(chunk(ep, c), chunk(ep, c), x_ssem.at[k, c], x_rsem.at[ep, c], {'ep': peer}) for k, peer in enumerate((across, mate))] for c in range(CHUNKS)]
    x_fwd = [remote(chunk(across, c), chunk(across, c), x_ssem.at[2, c], x_rsem.at[across, c], {'ep': mate}) for c in range(CHUNKS)]
    a_send = remote(attn_ref, attn_rx, a_sem.at[0], a_sem.at[1], {'tp': 1 - tp})
    start(g_sends)
    blocks = chunk_rows // block_rows
    for c in range(CHUNKS):
        lax.fori_loop(c * blocks, (c + 1) * blocks, attn_norm, 0, unroll=True)
        start(x_sends[c])

    def forward(c):
        recv_wait(chunk(across, c), x_rsem.at[across, c])
        x_fwd[c].start()

    lane = lax.broadcasted_iota(jnp.int32, (tokens, tokens), 1)
    row = lax.broadcasted_iota(jnp.int32, (tokens, tokens), 0)
    before = (row < lane).astype(jnp.bfloat16)
    slot_row = lax.broadcasted_iota(jnp.int32, (SLOT, tokens), 0).astype(jnp.float32)

    def dispatch(s, block):
        rows = pl.ds(pl.multiple_of(s * SLOT, SLOT), SLOT)
        gate = gates[s]
        chosen = (gate > 0.0).astype(jnp.float32)
        pos = jnp.dot(chosen.astype(jnp.bfloat16), before, preferred_element_type=jnp.float32)
        for j in range(n_local):
            hit = (pos[j:j + 1, :] == slot_row) & (chosen[j:j + 1, :] > 0.0)
            place[j * SLOT:(j + 1) * SLOT, :] = jnp.where(hit, 1.0, 0.0)
            picked = jnp.sum(jnp.where(hit, gate[j:j + 1, :], 0.0), axis=-1, keepdims=True)
            slot_gate[j, rows, :] = jnp.broadcast_to(picked, (SLOT, tokens))
        placed = place[...]
        place_t[s] = placed.T.astype(jnp.bfloat16)
        placed = placed.astype(jnp.bfloat16)

        for n in range(n_tiles):
            cols = slice(n * TILE, (n + 1) * TILE)
            got = jnp.dot(placed, block[:, cols], preferred_element_type=jnp.float32).astype(jnp.bfloat16)
            x_rows[:, rows, cols] = got.reshape(n_local, SLOT, TILE)

    x_own = x_ref[...]
    wait(proj)
    for n in range(qw // TILE):
        got = jnp.dot(x_own, ring[0, 0, :, n * TILE:(n + 1) * TILE], preferred_element_type=jnp.float32).astype(jnp.bfloat16).astype(jnp.float32)
        for k in range(TILE // HEAD):
            q_buf[:, n * (TILE // HEAD) + k, :] = got[:, k * HEAD:(k + 1) * HEAD]
    for n, buf in enumerate((k_buf, v_buf)):
        got = jnp.dot(x_own, ring[0, 1, :, n * kvw:(n + 1) * kvw], preferred_element_type=jnp.float32).astype(jnp.bfloat16).astype(jnp.float32)
        for k in range(n_heads):
            buf[:, k, :] = got[:, (k // group) * HEAD:(k // group + 1) * HEAD]

    scale = HEAD ** -0.5
    cache_lane = lax.broadcasted_iota(jnp.int32, (n_heads, ctx_rows), 1)
    head_row = lax.broadcasted_iota(jnp.int32, (n_heads, ctx_rows), 0)
    cache_pos = jnp.where(cache_lane % n_kv == head_row // group, cache_lane // n_kv, ctx_rows)

    def attend(i, carry):
        for c in range(CHUNKS // 2):
            @pl.when(i == n_batches - CHUNKS // 2 + c)
            def _(c=c):
                forward(c)

        first = i * BATCH
        base = (i % 2) * (BATCH // 2)
        wait(cache_copies(i, 0))

        def cache(u, n):
            return down[base + u // 2, (u % 2) * ctx_rows:(u % 2 + 1) * ctx_rows, n * HEAD:(n + 1) * HEAD]

        q_all = q_buf[pl.ds(pl.multiple_of(first, BATCH), BATCH)].reshape(BATCH * n_heads, HEAD).astype(jnp.bfloat16)
        stats = []
        for u in range(BATCH):
            t = first + u
            own_rows = slice(u * n_heads, (u + 1) * n_heads)
            s = lax.dot_general(q_all, cache(u, 0), (((1,), (1,)), ((), ())), preferred_element_type=jnp.float32)[own_rows] * scale
            s = jnp.where(cache_pos < len_ref[t], s, -jnp.inf)
            own = jnp.sum(q_buf[t] * k_buf[t], axis=-1, keepdims=True) * scale
            top = jnp.maximum(jnp.max(s, axis=-1, keepdims=True), own)
            w = jnp.exp(s - top)
            w_own = jnp.exp(own - top)
            p_buf[own_rows, :] = w
            stats.append((w_own, jnp.sum(w, axis=-1, keepdims=True) + w_own))

        @pl.when(i + 2 < n_batches)
        def _():
            start(cache_copies(i + 2, 0))

        wait(cache_copies(i, 1))
        p_all = p_buf[...].astype(jnp.bfloat16)
        for u in range(0, BATCH, 2):
            pair = jnp.concatenate([cache(u, 1), cache(u + 1, 1)], axis=1)
            mixed = jnp.dot(p_all, pair, preferred_element_type=jnp.float32)
            for e in range(2):
                w_own, norm = stats[u + e]
                mine = mixed[(u + e) * n_heads:(u + e + 1) * n_heads, e * HEAD:(e + 1) * HEAD]
                t = first + u + e
                o_buf[t] = (mine + w_own.astype(jnp.bfloat16).astype(jnp.float32) * v_buf[t]) / norm

        @pl.when(i + 2 < n_batches)
        def _():
            start(cache_copies(i + 2, 1))

        @pl.when(i == n_batches - 3)
        def _():
            start(expert_copies(0, 0))
            start(expert_copies(1, 1))
        return carry
    n_batches = tokens // BATCH
    lax.fori_loop(0, n_batches, attend, 0)
    down_start(0, 0)

    for k in range(n_heads):
        o_rows[:, k * HEAD:(k + 1) * HEAD] = o_buf[:, k, :].astype(jnp.bfloat16)
    out_proj.wait()
    for n in range(n_tiles):
        cols = slice(n * TILE, (n + 1) * TILE)
        got = jnp.dot(o_rows[...], x_rows[:, :, cols].reshape(qw, TILE), preferred_element_type=jnp.float32)
        attn_ref[:, cols] = got.astype(jnp.bfloat16)

    for c in range(CHUNKS // 2, CHUNKS):
        forward(c)

    gates[ep] = gt_ref[pl.ds(pl.multiple_of((ep * 2 + tp) * n_local, n_local), n_local), :]
    dispatch(ep, x_ref)
    for src in (mate, across, diagonal):
        recv_wait(gates.at[src], g_rsem.at[src])
    x_recv(mate)
    dispatch(mate, x_all.at[mate])
    a_send.start()
    dispatch(across, x_all.at[across])
    x_recv(diagonal)
    dispatch(diagonal, x_all.at[diagonal])

    def gate_up(lhs, slot, dst):
        full = hidden_dim // TILE * TILE
        for c in range(0, full, TILE):
            cols = slice(c, c + TILE)
            g = jnp.dot(lhs[...], ring[slot, 0, :, cols], preferred_element_type=jnp.float32)
            u = jnp.dot(lhs[...], ring[slot, 1, :, cols], preferred_element_type=jnp.float32)
            act[dst, :, cols] = (jax.nn.silu(g) * u).astype(jnp.bfloat16)
        if full < hidden_dim:
            cols = slice(full, hidden_dim)
            both = jnp.concatenate([ring[slot, 0, :, cols], ring[slot, 1, :, cols]], axis=1)
            gu = jnp.dot(lhs[...], both, preferred_element_type=jnp.float32)
            rest = hidden_dim - full
            act[dst, :, cols] = (jax.nn.silu(gu[:, :rest]) * gu[:, rest:]).astype(jnp.bfloat16)

    def expert(j, carry):
        slot = j % 2
        wait(expert_copies(j, slot))
        gate_up(x_rows.at[j], slot, j)

        @pl.when(j + 2 < n_local)
        def _():
            start(expert_copies(j + 2, slot))

        @pl.when(j + 2 == n_local)
        def _():
            start(shared_copies(slot))
        return carry
    lax.fori_loop(0, n_local, expert, 0)
    shared_slot = n_local % 2
    down_start(1, 1)

    recv_wait(attn_rx, a_sem.at[1])

    def ffn_norm(r, carry):
        rows = pl.ds(pl.multiple_of(r * block_rows, block_rows), block_rows)
        attn = (attn_ref[rows, :].astype(jnp.float32) + attn_rx[rows, :].astype(jnp.float32)).astype(jnp.bfloat16).astype(jnp.float32)
        res = h_ref[rows, :].astype(jnp.float32) + attn
        attn_sum[rows, :] = res
        y_norm[rows, :] = rms_norm(res, gain_f_ref[...]).astype(jnp.bfloat16)
        return carry
    lax.fori_loop(0, tokens // block_rows, ffn_norm, 0, unroll=4)
    wait(shared_copies(shared_slot))
    gate_up(y_norm, shared_slot, n_local)

    def split3(v):
        a = v.astype(jnp.bfloat16)
        r = v - a.astype(jnp.float32)
        b = r.astype(jnp.bfloat16)
        c = (r - b.astype(jnp.float32)).astype(jnp.bfloat16)
        return a, b, c

    def combine(s):
        rows = pl.ds(pl.multiple_of(s * SLOT, SLOT), SLOT)
        sums = [jnp.dot(place_t[s], y_parts[p, :, rows, :].reshape(n_local * SLOT, TILE), preferred_element_type=jnp.float32) for p in range(3)]
        return sums[0] + (sums[1] + sums[2])

    def s1_copy(i):
        return remote(send1.at[i], recv1.at[i], s1_sem.at[i], r1_sem.at[i], {'ep': mate})

    def s2_copy(i):
        return remote(send2.at[i], recv2.at[i], s2_sem.at[i], r2_sem.at[i], {'ep': across})

    def s3_copy(i):
        return remote(send3.at[i], recv3.at[i], s3_sem.at[i], r3_sem.at[i], {'tp': 1 - tp})

    def down_tile(i, slot, refill):
        base = slot * (n_local + 1)
        now = down_copies(i, slot)
        later = down_copies(i + 2, slot) if refill else None
        for k in range(len(now)):
            wait(now[k])
            for j in range(k * GROUP, min((k + 1) * GROUP, n_local)):
                out = jnp.dot(act[j], down[base + j], preferred_element_type=jnp.float32)
                parts = split3(out * jnp.concatenate([slot_gate[j]] * (TILE // tokens), axis=-1))
                for p in range(3):
                    y_parts[p, j] = parts[p]
            if k == len(now) - 1:
                keep_own[i] = jnp.dot(act[n_local], down[base + n_local], preferred_element_type=jnp.float32)

            if refill:
                start(later[k])
        for b in range(2):
            send1[i, b] = combine(b * 2 + 1 - core).astype(jnp.bfloat16)
        s1_copy(i).start()
        keep_other[i] = combine((1 - chip) * 2 + core)
        keep_own[i] = keep_own[i] + combine(ep)

    def step(i, carry, refill):
        if refill:
            down_tile(i, i % 2, True)
        else:
            @pl.when(i < n_tiles)
            def _():
                down_tile(i, i % 2, False)

        @pl.when((i >= LAG1) & (i < n_tiles + LAG1))
        def _():
            k = i - LAG1
            recv_wait(recv1.at[k], r1_sem.at[k])
            send2[k] = (keep_other[k] + recv1[k, 1 - chip].astype(jnp.float32)).astype(jnp.bfloat16)
            s2_copy(k).start()
            keep_own[k] = keep_own[k] + recv1[k, chip].astype(jnp.float32)

        @pl.when((i >= LAG2) & (i < n_tiles + LAG2))
        def _():
            k = i - LAG2
            recv_wait(recv2.at[k], r2_sem.at[k])
            send3[k] = (keep_own[k] + recv2[k].astype(jnp.float32)).astype(jnp.bfloat16)
            s3_copy(k).start()

        @pl.when(i >= LAG3)
        def _():
            k = i - LAG3
            cols = pl.ds(pl.multiple_of(k * TILE, TILE), TILE)
            recv_wait(recv3.at[k], r3_sem.at[k])
            ffn = send3[k].astype(jnp.float32) + recv3[k].astype(jnp.float32)
            out_ref[:, cols] = (attn_sum[:, cols] + ffn).astype(jnp.bfloat16)
        return carry
    lax.fori_loop(0, n_tiles - 2, functools.partial(step, refill=True), 0)
    lax.fori_loop(n_tiles - 2, n_tiles + LAG3, functools.partial(step, refill=False), 0)

    for c in g_sends + sum(x_sends, x_fwd) + [a_send]:
        c.wait_send()

    def drain(i, carry):
        s1_copy(i).wait_send()
        s2_copy(i).wait_send()
        s3_copy(i).wait_send()
        return carry
    lax.fori_loop(0, n_tiles, drain, 0)


def fused_layer(hidden, g_attn, w_q, w_k, w_v, w_o, k_cache, v_cache, lengths, g_ffn, ws_gate, ws_up, ws_down, w_gate, w_up, w_down, expert_ids, gate_vals, shards):
    tokens, d_model = hidden.shape
    n_local, _, hidden_dim = w_gate.shape
    n_tiles = d_model // TILE
    n_heads = w_q.shape[1] // HEAD
    ctx_len, n_kv = k_cache.shape[1:3]
    bf16, f32 = jnp.bfloat16, jnp.float32
    dma = pltpu.SemaphoreType.DMA
    hbm = pl.BlockSpec(memory_space=pltpu.HBM)
    tile = pltpu.VMEM((n_tiles, tokens, TILE), bf16)
    tile_f32 = pltpu.VMEM((n_tiles, tokens, TILE), f32)
    pair_tile = pltpu.VMEM((n_tiles, 2, tokens, TILE), bf16)
    rows_bf16 = pltpu.VMEM((tokens, d_model), bf16)
    heads = pltpu.VMEM((tokens, n_heads, HEAD), f32)
    caches = [c.reshape(tokens // 2, 2 * ctx_len * n_kv, HEAD) for c in (k_cache, v_cache)]
    return pl.pallas_call(
        layer_kernel,
        out_shape=pltpu.VMEM((tokens, d_model), bf16),
        in_specs=[hbm] * 18,
        out_specs=pl.BlockSpec(memory_space=pltpu.VMEM),
        scratch_shapes=[
            pltpu.VMEM((4, tokens, d_model), bf16),
            pltpu.VMEM((n_local, 4 * SLOT, d_model), bf16),
            pltpu.VMEM((n_local + 1, tokens, hidden_dim), bf16),
            pltpu.VMEM((4, tokens, n_local * SLOT), bf16),
            pltpu.VMEM((n_local, 4 * SLOT, tokens), f32),
            pltpu.VMEM((n_local * SLOT, tokens), f32),
            pltpu.VMEM((3, n_local, 4 * SLOT, TILE), bf16),
            pltpu.VMEM((2, 2, d_model, hidden_dim), bf16),
            pltpu.VMEM((2 * (n_local + 1), hidden_dim, TILE), bf16),
            rows_bf16, rows_bf16,
            pltpu.VMEM((tokens, d_model), f32),
            rows_bf16,
            pltpu.VMEM((4, n_local, tokens), f32),
            pltpu.VMEM((n_local * shards, tokens), f32),
            pltpu.SMEM((tokens,), jnp.int32), rows_bf16, pltpu.VMEM((1, d_model), f32), pltpu.VMEM((1, d_model), f32),
            pltpu.VMEM(expert_ids.shape[::-1], jnp.int32), pltpu.VMEM(gate_vals.shape[::-1], f32),
            heads, heads, heads, heads,
            pltpu.VMEM((BATCH * n_heads, ctx_len * n_kv), f32),
            pltpu.VMEM((tokens, n_heads * HEAD), bf16),
            pair_tile, pair_tile, tile, tile, tile, tile, tile_f32, tile_f32,
            dma((2, 2)), dma((2, 4)), dma((2, BATCH // 2, 2)), dma((4,)), dma((3, CHUNKS)), dma((4, CHUNKS)), dma((3,)), dma((4,)), dma((2,)),
        ] + [dma((n_tiles,))] * 6 + [dma((6,))],
        compiler_params=pltpu.CompilerParams(collective_id=0, has_side_effects=True, vmem_limit_bytes=63 * 1024 * 1024),
        cost_estimate=pl.CostEstimate(flops=2 * tokens * (n_local + 1) * 3 * d_model * hidden_dim, bytes_accessed=(n_local + 1) * 6 * d_model * hidden_dim, transcendentals=0),
        name='layer',
    )(lengths, hidden, g_attn.reshape(1, d_model), g_ffn.reshape(1, d_model), expert_ids.T, gate_vals.T, w_q, w_k, w_v, w_o.reshape(n_heads, HEAD, d_model), *caches, ws_gate, ws_up, ws_down, w_gate, w_up, w_down)


def solution(mesh):
    tok_spec = P(('rep', 'ep'), None)
    cache_spec = P(('rep', 'ep'), None, 'tp', None)
    expert_spec = P(('ep', 'tp'), None, None)
    layer = functools.partial(fused_layer, shards=mesh.shape['ep'] * mesh.shape['tp'])
    in_specs = (tok_spec, P(None), P(None, 'tp'), P(None, 'tp'), P(None, 'tp'), P('tp', None), cache_spec, cache_spec, P(('rep', 'ep')), P(None), P(None, 'tp'), P(None, 'tp'), P('tp', None), expert_spec, expert_spec, expert_spec, tok_spec, tok_spec)
    return jax.shard_map(layer, mesh=mesh, in_specs=in_specs, out_specs=tok_spec, check_vma=False)
```
